32 devices in a mesh: row: 8 (over y, x, core), col: 4 (over z).
Axes of the slice: x: 2, y: 2, z: 4, core: 2. Of those that a mesh axis runs over, the one named last changes fastest.
Arguments:
- history: float32 [3, 512, 4096], P(None, None, ('row', 'col')), may hold values from -8 to 8
Outputs:
- orbitals: float32 [512, 4096], P(None, ('row', 'col'))
The draws below stay inside these ranges and needn't reach their ends.
All inputs are finite; a program needn't handle non-finite values.
Results may differ from the reference program's by a relative error of at most 0.0003.
Values sent between devices are 32-bit elements; how exact they have to be, the bound alone decides.
No kernel may reach another device: no remote copies, remote signals or barrier semaphores. Data moves between devices by JAX's collectives and lax.ppermute only.
A program may use at most 64 MiB of HBM per device.

```python
import jax
import jax.numpy as jnp
from jax import lax

NORB = 512
NHIST = 3
NPW = 4096


def draw_history(key, part):
    base_key = jax.random.fold_in(key, 11)
    base = jax.random.truncated_normal(base_key, -4.0, 4.0, (NORB, NPW), jnp.float32)
    drifts = jax.random.truncated_normal(jax.random.fold_in(key, 13), -4.0, 4.0, (NHIST, NORB, NPW), jnp.float32)
    return base[None, :, :] + 0.35 * drifts


def setup_inputs(seed: int = 0) -> dict:
    splits = jax.random.split(jax.random.key(seed), 2)
    history = draw_history(jax.random.fold_in(splits[1], 71), 0)
    return {"history": history}


def reference(history):
    precise = lax.Precision.HIGHEST
    npw_total = history.shape[2]
    newest = history[0]
    weights = (2.5, -2.0, 0.5)
    predicted = jnp.zeros(newest.shape, jnp.float32)
    for index in range(3):
        project = jnp.einsum('ip,jp->ij', newest, history[index], precision=precise) / npw_total
        predicted = predicted + weights[index] * jnp.dot(project, history[index], precision=precise)
    gram = jnp.einsum('ip,jp->ij', predicted, predicted, precision=precise) / npw_total
    factor = jnp.linalg.cholesky(gram)
    return lax.linalg.triangular_solve(factor, predicted, left_side=True, lower=True)
```

```python
import functools

import jax
import jax.numpy as jnp
from jax import lax
from jax.experimental import pallas as pl
from jax.experimental.pallas import tpu as pltpu
from jax.sharding import PartitionSpec as P

HIGHEST = lax.Precision.HIGHEST
WEIGHTS = (2.5, -2.0, 0.5)
TILE = 128
PANEL = 32
GROUP = 16
AXES = ("row", "col")
NT = (((1,), (1,)), ((), ()))
NN = (((1,), (0,)), ((), ()))
TN = (((0,), (0,)), ((), ()))


def dot(a, b, dims):
    return lax.dot_general(a, b, dims, precision=HIGHEST, preferred_element_type=jnp.float32)


class Route:
    def __init__(self, mesh_rows, mesh_cols):
        self.rows, self.cols = mesh_rows, mesh_cols
        row_bits = list(range(1, mesh_rows.bit_length() - 1))
        col_bits = list(range(mesh_cols.bit_length() - 1))
        half = len(row_bits) // 2
        orders = (row_bits, row_bits[half:] + row_bits[:half])
        self.row_levels = len(row_bits)
        self.orders = tuple(
            [("row", b) for b in order] + [("col", b) for b in col_bits] for order in orders
        )
        self.levels = len(self.orders[0])

    def core_perm(self):
        c = self.cols
        return [(r * c + k, (r ^ 1) * c + k) for r in range(self.rows) for k in range(c)]

    def perm(self, level):
        pairs = []
        for r in range(self.rows):
            for k in range(self.cols):
                axis, bit = self.orders[r & 1][level]
                to = (r ^ (1 << bit), k) if axis == "row" else (r, k ^ (1 << bit))
                pairs.append((r * self.cols + k, to[0] * self.cols + to[1]))
        return pairs

    def place(self, core, levels):
        index = {"row": lax.axis_index("row"), "col": lax.axis_index("col")}
        numbers = []
        for order in self.orders:
            number = jnp.int32(0)
            for axis, bit in order[:levels]:
                number = number * 2 + ((index[axis] >> bit) & 1)
            numbers.append(number)
        return jnp.where(core == 0, numbers[0], numbers[1])


def swap(x, perm):
    return lax.ppermute(x, AXES, perm)


def all_reduce(route, keep, send, scatter, levels):
    for level in range(scatter):
        got = swap(send, route.perm(level))
        if level < scatter - 1:
            half = keep.shape[0] // 2
            keep, send = keep[:half] + got[:half], keep[half:] + got[half:]
        else:
            keep = keep + got
    for level in range(scatter, levels):
        keep = keep + swap(keep, route.perm(level))
    for level in reversed(range(scatter)):
        keep = jnp.concatenate([keep, swap(keep, route.perm(level))], axis=0)
    return keep


def project_kernel(blocks, where, own_ref, peer_ref, *refs):
    outs, (left, right) = refs[:-2], refs[-2:]
    rows, width = left.shape[0], own_ref.shape[2]
    core, place = where[0], where[1]
    size = rows // blocks
    for k in range(blocks):
        at = pl.multiple_of(core * rows + (place ^ k) * size, size)
        left[k * size : (k + 1) * size, :width] = own_ref[0, pl.ds(at, size), :]
        left[k * size : (k + 1) * size, width:] = peer_ref[0, pl.ds(at, size), :]
    for j in range(own_ref.shape[0]):
        right[:, :width] = own_ref[j]
        right[:, width:] = peer_ref[j]
        keep, send = outs[2 * j], outs[2 * j + 1]
        half = keep.shape[0]
        keep[...] = dot(left[:half, :], right[...], NT)
        send[...] = dot(left[half:, :], right[...], NT)


def predict_kernel(blocks, scales, where, m0, m1, m2, own_ref, peer_ref, out_ref, both, acc):
    rows, width = m0.shape[0], own_ref.shape[2]
    size = rows // blocks
    for j, m in enumerate((m0, m1, m2)):
        both[:, :width] = own_ref[j]
        both[:, width:] = peer_ref[j]
        term = dot(m[...], both[...], NN) * scales[j]
        if j == 0:
            acc[...] = term
        else:
            acc[...] += term
    place = where[1]
    for k in range(blocks):
        at = pl.multiple_of((place ^ k) * size, size)
        out_ref[pl.ds(at, size), :] = acc[k * size : (k + 1) * size, :]


def core_blocks(count):
    blocks = [(i, j) for i in range(count) for j in range(i, count)]
    half = (len(blocks) + 1) // 2
    return blocks[:half], blocks[half:]


def gram_kernel(parts, scale, where, p_ref, keep_ref, send_ref, acc):
    count = p_ref.shape[0] // TILE
    lists = core_blocks(count)
    core, place = where[0], where[1]
    for n in range(len(lists[0])):
        first = lists[0][n]
        second = lists[1][min(n, len(lists[1]) - 1)]
        i = jnp.where(core == 0, first[0], second[0])
        j = jnp.where(core == 0, first[1], second[1])
        a = p_ref[pl.ds(pl.multiple_of(i * TILE, TILE), TILE), :]
        b = p_ref[pl.ds(pl.multiple_of(j * TILE, TILE), TILE), :]
        acc[n * TILE : (n + 1) * TILE, :] = dot(a, b, NT) * scale
    size = acc.shape[0] // parts
    for k in range(parts):
        rows = acc[pl.ds(pl.multiple_of((place ^ k) * size, 8), size), :]
        if k < parts // 2:
            keep_ref[k * size : (k + 1) * size, :] = rows
        else:
            send_ref[(k - parts // 2) * size : (k - parts // 2 + 1) * size, :] = rows


def solve_kernel(parts, where, mine_ref, other_ref, p_ref, out_ref, natural, work):
    n, tile = p_ref.shape[0], TILE
    width = n + out_ref.shape[1]
    count, groups, per_panel, panels = n // tile, width // tile, PANEL // 8, tile // PANEL
    core, size = where[0], mine_ref.shape[0] // parts
    for ref, number, place in ((mine_ref, core, where[1]), (other_ref, 1 - core, where[2])):
        for k in range(parts):
            at = pl.multiple_of((place ^ k) * size, 8)
            natural[number, pl.ds(at, size), :] = ref[k * size : (k + 1) * size, :]
    for number, blocks in enumerate(core_blocks(count)):
        for at, (i, j) in enumerate(blocks):
            work[i * tile : (i + 1) * tile, j * tile : (j + 1) * tile] = natural[number, at * tile : (at + 1) * tile, :]
    work[:, n:] = p_ref[:, : out_ref.shape[1]]
    sub = lax.broadcasted_iota(jnp.int32, (8, tile), 0)

    def panel(r0, s):
        base = r0 + PANEL * s
        r = [
            [work[pl.ds(base + 8 * i, 8), c * tile : (c + 1) * tile] for c in range(groups)]
            + [work[pl.ds(base + 8 * i, 8), pl.ds(r0, tile)]]
            for i in range(per_panel)
        ]
        scale = [jnp.zeros((8, tile), jnp.float32)] * per_panel
        cols = {}
        for j in range(PANEL):
            if j % GROUP == 0:
                cols = {
                    k: {
                        i: jnp.broadcast_to(r[i][groups][:, PANEL * s + k : PANEL * s + k + 1], (8, tile))
                        for i in range(k // 8, per_panel)
                    }
                    for k in range(j, j + GROUP)
                }
            jb, js = j // 8, j % 8
            col = cols[j]
            pivot = jnp.broadcast_to(col[jb][js : js + 1, :], (8, tile))
            scale[jb] = jnp.where(sub == js, lax.rsqrt(pivot), scale[jb])
            inverse = 1.0 / pivot
            mult = {i: col[i] * inverse for i in range(jb, per_panel)}
            mult[jb] = jnp.where(sub > js, mult[jb], 0.0)
            first = jb if js < 7 else jb + 1
            for k in range(j + 1, (j // GROUP + 1) * GROUP):
                row = jnp.broadcast_to(col[k // 8][k % 8 : k % 8 + 1, :], (8, tile))
                for i in range(k // 8, per_panel):
                    cols[k][i] = cols[k][i] - mult[i] * row
            for c in range(groups + 1):
                row = jnp.broadcast_to(r[jb][c][js : js + 1, :], (8, tile))
                for i in range(first, per_panel):
                    r[i][c] = r[i][c] - mult[i] * row
        for i in range(per_panel):
            for c in range(groups):
                work[pl.ds(base + 8 * i, 8), c * tile : (c + 1) * tile] = r[i][c] * scale[i]
        return jnp.concatenate([r[i][groups] * scale[i] for i in range(per_panel)], axis=0)

    def block(b, carry):
        r0 = pl.multiple_of(b * tile, tile)
        for s in range(panels):
            left = panel(r0, s)
            if s < panels - 1:
                low = PANEL * (s + 1)
                update = dot(left, work[pl.ds(r0 + PANEL * s, PANEL), :], TN)
                work[pl.ds(r0 + low, tile - low), :] -= update[low:, :]

        def trail(i, inner):
            at = pl.multiple_of(i * tile, tile)
            work[pl.ds(at, tile), :] -= dot(work[pl.ds(r0, tile), pl.ds(at, tile)], work[pl.ds(r0, tile), :], TN)
            return inner

        lax.fori_loop(b + 1, count, trail, 0)
        return carry

    lax.fori_loop(0, count, block, 0)
    out_ref[...] = work[:, n:]


VMEM = pl.BlockSpec(memory_space=pltpu.VMEM)
SMEM = pl.BlockSpec(memory_space=pltpu.SMEM)


def f32(*shape):
    return jax.ShapeDtypeStruct(shape, jnp.float32)


def call(kernel, name, out_shape, scratch, *args):
    return pl.pallas_call(
        kernel,
        name=name,
        out_shape=out_shape,
        in_specs=[SMEM] + [VMEM] * (len(args) - 1),
        out_specs=jax.tree.map(lambda _: VMEM, out_shape),
        scratch_shapes=[pltpu.VMEM(s.shape, s.dtype) for s in scratch],
    )(*args)


def on_device(rows, cols, history):
    route = Route(rows, cols)
    terms, norb, width = history.shape
    total = width * rows * cols
    half = norb // 2
    core = lax.axis_index("row") & 1

    levels = route.levels
    scatter = min(levels, (half // 8).bit_length() - 1)
    blocks = 1 << scatter
    where_m = jnp.stack([core, route.place(core, scatter)])
    parts_levels = route.row_levels
    parts = 1 << parts_levels
    where_g = jnp.stack([core, route.place(core, parts_levels), route.place(1 - core, parts_levels)])

    peer = swap(history, route.core_perm())
    quarter = half // 2
    products = call(
        functools.partial(project_kernel, blocks),
        "project",
        [f32(quarter, norb)] * (2 * terms),
        [f32(half, 2 * width), f32(norb, 2 * width)],
        where_m,
        history,
        peer,
    )
    m = [all_reduce(route, products[2 * j], products[2 * j + 1], scatter, levels) for j in range(terms)]
    mine = call(
        functools.partial(predict_kernel, blocks, tuple(w / total for w in WEIGHTS)),
        "predict",
        f32(half, 2 * width),
        [f32(norb, 2 * width), f32(half, 2 * width)],
        where_m,
        *m,
        history,
        peer,
    )
    other = swap(mine, route.core_perm())
    other = jnp.concatenate([other[:, width:], other[:, :width]], axis=1)
    predicted = jnp.where(core == 0, jnp.concatenate([mine, other]), jnp.concatenate([other, mine]))

    shares = (norb // TILE) * (norb // TILE + 1) // 2
    share = (shares + 1) // 2 * TILE
    keep, send = call(
        functools.partial(gram_kernel, parts, 1.0 / total),
        "gram",
        [f32(share // 2, TILE)] * 2,
        [f32(share, TILE)],
        where_g,
        predicted,
    )
    gram = all_reduce(route, keep, send, parts_levels, levels)
    gram_other = swap(gram, route.core_perm())
    return call(
        functools.partial(solve_kernel, parts),
        "solve",
        f32(norb, width),
        [f32(2, share, TILE), f32(norb, norb + width)],
        where_g,
        gram,
        gram_other,
        predicted,
    )


def solution(mesh):
    return jax.shard_map(
        functools.partial(on_device, mesh.shape["row"], mesh.shape["col"]),
        mesh=mesh,
        in_specs=(P(None, None, ("row", "col")),),
        out_specs=P(None, ("row", "col")),
        check_vma=False,
    )
```

```python
import functools

import jax
import jax.numpy as jnp
from jax import lax
from jax.experimental import pallas as pl
from jax.experimental.pallas import tpu as pltpu
from jax.sharding import PartitionSpec as P

HIGHEST = lax.Precision.HIGHEST
WEIGHTS = (2.5, -2.0, 0.5)
TILE = 128
PANEL = 32
GROUP = 16
VMEM_LIMIT = 16 << 20
AXES = ("row", "col")
NT = (((1,), (1,)), ((), ()))
NN = (((1,), (0,)), ((), ()))
TN = (((0,), (0,)), ((), ()))


def dot(a, b, dims):
    return lax.dot_general(a, b, dims, precision=HIGHEST, preferred_element_type=jnp.float32)


def bf16_dot(a, b, dims):
    return lax.dot_general(a, b, dims, preferred_element_type=jnp.float32)


def split(x):
    high = x.astype(jnp.bfloat16)
    rest = x - high.astype(jnp.float32)
    middle = rest.astype(jnp.bfloat16)
    return high, middle, (rest - middle.astype(jnp.float32)).astype(jnp.bfloat16)


def stacked(x, axis):
    h, m, low = split(x)
    return jnp.concatenate([h, h, m, h, low, m], axis=axis), jnp.concatenate([h, m, h, low, h, m], axis=axis)


class Route:
    def __init__(self, mesh_rows, mesh_cols):
        self.rows, self.cols = mesh_rows, mesh_cols
        row_bits = list(range(1, mesh_rows.bit_length() - 1))
        col_bits = list(range(mesh_cols.bit_length() - 1))
        half = len(row_bits) // 2
        orders = (row_bits, row_bits[half:] + row_bits[:half])
        self.row_levels = len(row_bits)
        self.orders = tuple(
            [("row", b) for b in order] + [("col", b) for b in col_bits] for order in orders
        )
        self.levels = len(self.orders[0])

    def core_perm(self):
        c = self.cols
        return [(r * c + k, (r ^ 1) * c + k) for r in range(self.rows) for k in range(c)]

    def perm(self, level):
        pairs = []
        for r in range(self.rows):
            for k in range(self.cols):
                axis, bit = self.orders[r & 1][level]
                to = (r ^ (1 << bit), k) if axis == "row" else (r, k ^ (1 << bit))
                pairs.append((r * self.cols + k, to[0] * self.cols + to[1]))
        return pairs

    def place(self, core, levels):
        index = {"row": lax.axis_index("row"), "col": lax.axis_index("col")}
        numbers = []
        for order in self.orders:
            number = jnp.int32(0)
            for axis, bit in order[:levels]:
                number = number * 2 + ((index[axis] >> bit) & 1)
            numbers.append(number)
        return jnp.where(core == 0, numbers[0], numbers[1])


def swap(x, perm):
    return lax.ppermute(x, AXES, perm)


def all_reduce(route, keep, send, scatter, levels):
    for level in range(scatter):
        got = swap(send, route.perm(level))
        if level < scatter - 1:
            half = keep.shape[0] // 2
            keep, send = keep[:half] + got[:half], keep[half:] + got[half:]
        else:
            keep = keep + got
    for level in range(scatter, levels):
        keep = keep + swap(keep, route.perm(level))
    for level in reversed(range(scatter)):
        keep = jnp.concatenate([keep, swap(keep, route.perm(level))], axis=0)
    return keep


def project_kernel(blocks, where, own_ref, peer_ref, *refs):
    outs, (left, right) = refs[:-2], refs[-2:]
    rows, width = left.shape[0], own_ref.shape[2]
    core, place = where[0], where[1]
    size = rows // blocks
    for k in range(blocks):
        at = pl.multiple_of(core * rows + (place ^ k) * size, size)
        left[k * size : (k + 1) * size, :width] = own_ref[0, pl.ds(at, size), :]
        left[k * size : (k + 1) * size, width:] = peer_ref[0, pl.ds(at, size), :]
    for j in range(own_ref.shape[0]):
        right[:, :width] = own_ref[j]
        right[:, width:] = peer_ref[j]
        keep, send = outs[2 * j], outs[2 * j + 1]
        half = keep.shape[0]
        keep[...] = dot(left[:half, :], right[...], NT)
        send[...] = dot(left[half:, :], right[...], NT)


def predict_kernel(blocks, scales, where, m0, m1, m2, own_ref, peer_ref, out_ref, both, acc):
    rows, width = m0.shape[0], own_ref.shape[2]
    size = rows // blocks
    for j, m in enumerate((m0, m1, m2)):
        both[:, :width] = own_ref[j]
        both[:, width:] = peer_ref[j]
        term = dot(m[...], both[...], NN) * scales[j]
        if j == 0:
            acc[...] = term
        else:
            acc[...] += term
    place = where[1]
    for k in range(blocks):
        at = pl.multiple_of((place ^ k) * size, size)
        out_ref[pl.ds(at, size), :] = acc[k * size : (k + 1) * size, :]


def core_blocks(count):
    blocks = [(i, j) for i in range(count) for j in range(i, count)]
    half = (len(blocks) + 1) // 2
    return blocks[:half], blocks[half:]


def gram_kernel(parts, scale, where, mine_ref, other_ref, keep_ref, send_ref, own_ref, p, acc):
    half, width = mine_ref.shape[0], own_ref.shape[1]
    count = 2 * half // TILE
    lists = core_blocks(count)
    core, place = where[0], where[1]
    here = pl.ds(pl.multiple_of(core * half, half), half)
    there = pl.ds(pl.multiple_of((1 - core) * half, half), half)
    p[here, :] = mine_ref[...]
    p[there, :width] = other_ref[:, width:]
    p[there, width:] = other_ref[:, :width]
    own_ref[...] = p[:, :width]
    for n in range(len(lists[0])):
        first = lists[0][n]
        second = lists[1][min(n, len(lists[1]) - 1)]
        i = jnp.where(core == 0, first[0], second[0])
        j = jnp.where(core == 0, first[1], second[1])
        a = p[pl.ds(pl.multiple_of(i * TILE, TILE), TILE), :]
        b = p[pl.ds(pl.multiple_of(j * TILE, TILE), TILE), :]
        acc[n * TILE : (n + 1) * TILE, :] = dot(a, b, NT) * scale
    size = acc.shape[0] // parts
    for k in range(parts):
        rows = acc[pl.ds(pl.multiple_of((place ^ k) * size, 8), size), :]
        if k < parts // 2:
            keep_ref[k * size : (k + 1) * size, :] = rows
        else:
            send_ref[(k - parts // 2) * size : (k - parts // 2 + 1) * size, :] = rows


def solve_kernel(parts, where, mine_ref, other_ref, p_ref, out_ref, natural, work, stack_a, stack_b):
    n, tile = p_ref.shape[0], TILE
    width = n + p_ref.shape[1]
    count, groups, per_panel, panels = n // tile, width // tile, PANEL // 8, tile // PANEL
    core, size = where[0], mine_ref.shape[0] // parts
    for ref, number, place in ((mine_ref, core, where[1]), (other_ref, 1 - core, where[2])):
        for k in range(parts):
            at = pl.multiple_of((place ^ k) * size, 8)
            natural[number, pl.ds(at, size), :] = ref[k * size : (k + 1) * size, :]
    for number, blocks in enumerate(core_blocks(count)):
        for at, (i, j) in enumerate(blocks):
            work[i * tile : (i + 1) * tile, j * tile : (j + 1) * tile] = natural[number, at * tile : (at + 1) * tile, :]
    work[:, n:] = p_ref[...]
    sub = lax.broadcasted_iota(jnp.int32, (8, tile), 0)
    deep = 6 * PANEL

    def panel(b, s):
        base = b * tile + PANEL * s
        r = [
            [work[base + 8 * i : base + 8 * i + 8, c * tile : (c + 1) * tile] for c in range(b, groups)]
            for i in range(per_panel)
        ]
        scale = [jnp.zeros((8, tile), jnp.float32)] * per_panel
        cols = {}
        for j in range(PANEL):
            if j % GROUP == 0:
                cols = {
                    k: {
                        i: jnp.broadcast_to(r[i][0][:, PANEL * s + k : PANEL * s + k + 1], (8, tile))
                        for i in range(k // 8, per_panel)
                    }
                    for k in range(j, j + GROUP)
                }
            jb, js = j // 8, j % 8
            col = cols[j]
            pivot = jnp.broadcast_to(col[jb][js : js + 1, :], (8, tile))
            scale[jb] = jnp.where(sub == js, lax.rsqrt(pivot), scale[jb])
            inverse = 1.0 / pivot
            mult = {i: col[i] * inverse for i in range(jb, per_panel)}
            mult[jb] = jnp.where(sub > js, mult[jb], 0.0)
            first = jb if js < 7 else jb + 1
            for k in range(j + 1, (j // GROUP + 1) * GROUP):
                row = jnp.broadcast_to(col[k // 8][k % 8 : k % 8 + 1, :], (8, tile))
                for i in range(k // 8, per_panel):
                    cols[k][i] = cols[k][i] - mult[i] * row
            for c in range(groups - b):
                row = jnp.broadcast_to(r[jb][c][js : js + 1, :], (8, tile))
                for i in range(first, per_panel):
                    r[i][c] = r[i][c] - mult[i] * row
        return jnp.concatenate(
            [jnp.concatenate([x * scale[i] for x in r[i]], axis=1) for i in range(per_panel)], axis=0
        )

    for b in range(count):
        start = b * tile
        for s in range(panels):
            u = panel(b, s)
            out_ref[start + PANEL * s : start + PANEL * (s + 1), :] = u[:, n - start :]
            if b == count - 1 and s == panels - 1:
                break
            left, right = stacked(u, axis=0)
            if s < panels - 1:
                low = PANEL * (s + 1)
                update = bf16_dot(left[:, :tile], right, TN)
                work[start + low : start + tile, start:] -= update[low:, :]
            if b < count - 1:
                stack_a[deep * s : deep * (s + 1), start:n] = left[:, : n - start]
                stack_b[deep * s : deep * (s + 1), start:] = right
        for i in range(b + 1, count):
            at = i * tile
            work[at : at + tile, at:] -= bf16_dot(stack_a[:, at : at + tile], stack_b[:, at:], TN)


VMEM = pl.BlockSpec(memory_space=pltpu.VMEM)
SMEM = pl.BlockSpec(memory_space=pltpu.SMEM)


def f32(*shape):
    return jax.ShapeDtypeStruct(shape, jnp.float32)


def call(kernel, name, out_shape, scratch, *args):
    return pl.pallas_call(
        kernel,
        name=name,
        out_shape=out_shape,
        in_specs=[SMEM] + [VMEM] * (len(args) - 1),
        out_specs=jax.tree.map(lambda _: VMEM, out_shape),
        scratch_shapes=[pltpu.VMEM(s.shape, s.dtype) for s in scratch],
        compiler_params=pltpu.CompilerParams(vmem_limit_bytes=VMEM_LIMIT),
    )(*args)


def on_device(rows, cols, history):
    route = Route(rows, cols)
    terms, norb, width = history.shape
    total = width * rows * cols
    half = norb // 2
    core = lax.axis_index("row") & 1

    levels = route.levels
    scatter = min(levels, (half // 8).bit_length() - 1)
    blocks = 1 << scatter
    where_m = jnp.stack([core, route.place(core, scatter)])
    parts_levels = route.row_levels
    parts = 1 << parts_levels
    where_g = jnp.stack([core, route.place(core, parts_levels), route.place(1 - core, parts_levels)])

    peer = swap(history, route.core_perm())
    quarter = half // 2
    products = call(
        functools.partial(project_kernel, blocks),
        "project",
        [f32(quarter, norb)] * (2 * terms),
        [f32(half, 2 * width), f32(norb, 2 * width)],
        where_m,
        history,
        peer,
    )
    m = [all_reduce(route, products[2 * j], products[2 * j + 1], scatter, levels) for j in range(terms)]
    mine = call(
        functools.partial(predict_kernel, blocks, tuple(w / total for w in WEIGHTS)),
        "predict",
        f32(half, 2 * width),
        [f32(norb, 2 * width), f32(half, 2 * width)],
        where_m,
        *m,
        history,
        peer,
    )
    other = swap(mine, route.core_perm())

    shares = (norb // TILE) * (norb // TILE + 1) // 2
    share = (shares + 1) // 2 * TILE
    keep, send, predicted = call(
        functools.partial(gram_kernel, parts, 1.0 / total),
        "gram",
        [f32(share // 2, TILE)] * 2 + [f32(norb, width)],
        [f32(norb, 2 * width), f32(share, TILE)],
        where_g,
        mine,
        other,
    )
    gram = all_reduce(route, keep, send, parts_levels, levels)
    gram_other = swap(gram, route.core_perm())
    return call(
        functools.partial(solve_kernel, parts),
        "solve",
        f32(norb, width),
        [
            f32(2, share, TILE),
            f32(norb, norb + width),
            jax.ShapeDtypeStruct((6 * TILE, norb), jnp.bfloat16),
            jax.ShapeDtypeStruct((6 * TILE, norb + width), jnp.bfloat16),
        ],
        where_g,
        gram,
        gram_other,
        predicted,
    )


def solution(mesh):
    return jax.shard_map(
        functools.partial(on_device, mesh.shape["row"], mesh.shape["col"]),
        mesh=mesh,
        in_specs=(P(None, None, ("row", "col")),),
        out_specs=P(None, ("row", "col")),
        check_vma=False,
    )
```

```python
import functools

import jax
import jax.numpy as jnp
from jax import lax
from jax.experimental import pallas as pl
from jax.experimental.pallas import tpu as pltpu
from jax.sharding import PartitionSpec as P

HIGHEST = lax.Precision.HIGHEST
WEIGHTS = (2.5, -2.0, 0.5)
TILE = 128
PANEL = 32
GROUP = 16
VMEM_LIMIT = 16 << 20
AXES = ("row", "col")
NT = (((1,), (1,)), ((), ()))
NN = (((1,), (0,)), ((), ()))
TN = (((0,), (0,)), ((), ()))


def dot(a, b, dims):
    return lax.dot_general(a, b, dims, precision=HIGHEST, preferred_element_type=jnp.float32)


def bf16_dot(a, b, dims):
    return lax.dot_general(a, b, dims, preferred_element_type=jnp.float32)


def split(x):
    high = x.astype(jnp.bfloat16)
    rest = x - high.astype(jnp.float32)
    middle = rest.astype(jnp.bfloat16)
    return high, middle, (rest - middle.astype(jnp.float32)).astype(jnp.bfloat16)


def stacked(x, axis):
    h, m, low = split(x)
    return jnp.concatenate([h, h, m, h, low, m], axis=axis), jnp.concatenate([h, m, h, low, h, m], axis=axis)


class Route:
    def __init__(self, mesh_rows, mesh_cols):
        self.rows, self.cols = mesh_rows, mesh_cols
        row_bits = list(range(1, mesh_rows.bit_length() - 1))
        col_bits = list(range(mesh_cols.bit_length() - 1))
        half = len(row_bits) // 2
        orders = (row_bits, row_bits[half:] + row_bits[:half])
        self.row_levels = len(row_bits)
        self.orders = tuple(
            [("row", b) for b in order] + [("col", b) for b in col_bits] for order in orders
        )
        self.levels = len(self.orders[0])

    def core_perm(self):
        c = self.cols
        return [(r * c + k, (r ^ 1) * c + k) for r in range(self.rows) for k in range(c)]

    def perm(self, *levels):
        pairs = []
        for r in range(self.rows):
            for k in range(self.cols):
                flip = {"row": 0, "col": 0}
                for level in levels:
                    axis, bit = self.orders[r & 1][level]
                    flip[axis] ^= 1 << bit
                pairs.append((r * self.cols + k, (r ^ flip["row"]) * self.cols + (k ^ flip["col"])))
        return pairs

    def perms(self, first, count):
        return [
            self.perm(*[first + i for i in range(count) if q >> (count - 1 - i) & 1]) for q in range(1, 1 << count)
        ]

    def place(self, core, levels):
        index = {"row": lax.axis_index("row"), "col": lax.axis_index("col")}
        numbers = []
        for order in self.orders:
            number = jnp.int32(0)
            for axis, bit in order[:levels]:
                number = number * 2 + ((index[axis] >> bit) & 1)
            numbers.append(number)
        return jnp.where(core == 0, numbers[0], numbers[1])


def swap(x, perm):
    return lax.ppermute(x, AXES, perm)


def all_reduce(route, keep, send, scatter, levels):
    for level in range(scatter):
        got = swap(send, route.perm(level))
        if level < scatter - 1:
            half = keep.shape[0] // 2
            keep, send = keep[:half] + got[:half], keep[half:] + got[half:]
        else:
            keep = keep + got
    for level in range(scatter, levels):
        keep = keep + swap(keep, route.perm(level))
    for level in reversed(range(scatter)):
        keep = jnp.concatenate([keep, swap(keep, route.perm(level))], axis=0)
    return keep


def phases(first, last):
    return [(level, min(2, last - level)) for level in range(first, last, 2)]


def direct_all_reduce(route, pieces, scatter, levels):
    for number, (level, count) in enumerate(phases(0, scatter)):
        if number > 0:
            size = keep.shape[0] >> count
            pieces = [keep[q * size : (q + 1) * size] for q in range(1 << count)]
        got = [swap(piece, perm) for piece, perm in zip(pieces[1:], route.perms(level, count))]
        keep = functools.reduce(jnp.add, got, pieces[0])
    for level, count in phases(scatter, levels):
        keep = functools.reduce(jnp.add, [swap(keep, perm) for perm in route.perms(level, count)], keep)
    for level, count in reversed(phases(0, scatter)):
        keep = jnp.concatenate([keep] + [swap(keep, perm) for perm in route.perms(level, count)])
    return keep


def arrange_kernel(blocks, where, own_ref, peer_ref, out_ref, left):
    rows, width = left.shape[0], own_ref.shape[1]
    core, place = where[0], where[1]
    size = rows // blocks
    for k in range(blocks):
        at = pl.multiple_of(core * rows + (place ^ k) * size, size)
        left[k * size : (k + 1) * size, :width] = own_ref[pl.ds(at, size), :]
        left[k * size : (k + 1) * size, width:] = peer_ref[pl.ds(at, size), :]
    out_ref[...] = stacked(left[...], axis=1)[0]


def project_kernel(left_ref, own_ref, peer_ref, keep_ref, send_ref):
    half = keep_ref.shape[0]
    right = stacked(jnp.concatenate([own_ref[...], peer_ref[...]], axis=1), axis=1)[1]
    keep_ref[...] = bf16_dot(left_ref[:half, :], right, NT)
    send_ref[...] = bf16_dot(left_ref[half:, :], right, NT)


def predict_kernel(scale, m_ref, own_ref, peer_ref, *refs):
    out_ref = refs[-1]
    left = stacked(m_ref[...], axis=1)[0]
    right = stacked(jnp.concatenate([own_ref[...], peer_ref[...]], axis=1), axis=0)[1]
    term = bf16_dot(left, right, NN) * scale
    out_ref[...] = term + refs[0][...] if len(refs) > 1 else term


def core_blocks(count):
    blocks = [(i, j) for i in range(count) for j in range(i, count)]
    half = (len(blocks) + 1) // 2
    return blocks[:half], blocks[half:]


def restore_kernel(blocks, where, in_ref, out_ref):
    size = in_ref.shape[0] // blocks
    for k in range(blocks):
        out_ref[pl.ds(pl.multiple_of((where[1] ^ k) * size, size), size), :] = in_ref[k * size : (k + 1) * size, :]


def gram_kernel(parts, scale, where, mine_ref, other_ref, *refs):
    outs, own_ref, p, acc = refs[:-3], refs[-3], refs[-2], refs[-1]
    half, width = mine_ref.shape[0], own_ref.shape[1]
    count = 2 * half // TILE
    lists = core_blocks(count)
    core, place = where[0], where[1]
    here = pl.ds(pl.multiple_of(core * half, half), half)
    there = pl.ds(pl.multiple_of((1 - core) * half, half), half)
    p[here, :] = mine_ref[...]
    p[there, :width] = other_ref[:, width:]
    p[there, width:] = other_ref[:, :width]
    own_ref[...] = p[:, :width]
    for n in range(len(lists[0])):
        first = lists[0][n]
        second = lists[1][min(n, len(lists[1]) - 1)]
        i = jnp.where(core == 0, first[0], second[0])
        j = jnp.where(core == 0, first[1], second[1])
        a = p[pl.ds(pl.multiple_of(i * TILE, TILE), TILE), :]
        b = p[pl.ds(pl.multiple_of(j * TILE, TILE), TILE), :]
        acc[n * TILE : (n + 1) * TILE, :] = dot(a, b, NT) * scale
    size = acc.shape[0] // parts
    for k in range(parts):
        each = parts // len(outs)
        outs[k // each][k % each * size : (k % each + 1) * size, :] = acc[pl.ds(pl.multiple_of((place ^ k) * size, 8), size), :]


def solve_kernel(parts, where, mine_ref, other_ref, p_ref, out_ref, natural, work, stack_a, stack_b):
    n, tile = p_ref.shape[0], TILE
    width = n + p_ref.shape[1]
    count, groups, per_panel, panels = n // tile, width // tile, PANEL // 8, tile // PANEL
    core, size = where[0], mine_ref.shape[0] // parts
    for ref, number, place in ((mine_ref, core, where[1]), (other_ref, 1 - core, where[2])):
        for k in range(parts):
            at = pl.multiple_of((place ^ k) * size, 8)
            natural[number, pl.ds(at, size), :] = ref[k * size : (k + 1) * size, :]
    for number, blocks in enumerate(core_blocks(count)):
        for at, (i, j) in enumerate(blocks):
            work[i * tile : (i + 1) * tile, j * tile : (j + 1) * tile] = natural[number, at * tile : (at + 1) * tile, :]
    work[:, n:] = p_ref[...]
    sub = lax.broadcasted_iota(jnp.int32, (8, tile), 0)
    deep = 6 * PANEL

    def panel(b, s):
        base = b * tile + PANEL * s
        r = [
            [work[base + 8 * i : base + 8 * i + 8, c * tile : (c + 1) * tile] for c in range(b, groups)]
            for i in range(per_panel)
        ]
        scale = [jnp.zeros((8, tile), jnp.float32)] * per_panel
        cols = {}
        for j in range(PANEL):
            if j % GROUP == 0:
                cols = {
                    k: {
                        i: jnp.broadcast_to(r[i][0][:, PANEL * s + k : PANEL * s + k + 1], (8, tile))
                        for i in range(k // 8, per_panel)
                    }
                    for k in range(j, j + GROUP)
                }
            jb, js = j // 8, j % 8
            col = cols[j]
            pivot = jnp.broadcast_to(col[jb][js : js + 1, :], (8, tile))
            scale[jb] = jnp.where(sub == js, lax.rsqrt(pivot), scale[jb])
            inverse = 1.0 / pivot
            mult = {i: col[i] * inverse for i in range(jb, per_panel)}
            mult[jb] = jnp.where(sub > js, mult[jb], 0.0)
            first = jb if js < 7 else jb + 1
            for k in range(j + 1, (j // GROUP + 1) * GROUP):
                row = jnp.broadcast_to(col[k // 8][k % 8 : k % 8 + 1, :], (8, tile))
                for i in range(k // 8, per_panel):
                    cols[k][i] = cols[k][i] - mult[i] * row
            for c in range(groups - b):
                row = jnp.broadcast_to(r[jb][c][js : js + 1, :], (8, tile))
                for i in range(first, per_panel):
                    r[i][c] = r[i][c] - mult[i] * row
        return jnp.concatenate(
            [jnp.concatenate([x * scale[i] for x in r[i]], axis=1) for i in range(per_panel)], axis=0
        )

    for b in range(count):
        start = b * tile
        for s in range(panels):
            u = panel(b, s)
            out_ref[start + PANEL * s : start + PANEL * (s + 1), :] = u[:, n - start :]
            if b == count - 1 and s == panels - 1:
                break
            left, right = stacked(u, axis=0)
            if s < panels - 1:
                low = PANEL * (s + 1)
                update = bf16_dot(left[:, :tile], right, TN)
                work[start + low : start + tile, start:] -= update[low:, :]
            if b < count - 1:
                stack_a[deep * s : deep * (s + 1), start:n] = left[:, : n - start]
                stack_b[deep * s : deep * (s + 1), start:] = right
        for i in range(b + 1, count):
            at = i * tile
            work[at : at + tile, at:] -= bf16_dot(stack_a[:, at : at + tile], stack_b[:, at:], TN)


VMEM = pl.BlockSpec(memory_space=pltpu.VMEM)
SMEM = pl.BlockSpec(memory_space=pltpu.SMEM)


def f32(*shape):
    return jax.ShapeDtypeStruct(shape, jnp.float32)


def call(kernel, name, out_shape, scratch, args, scalars=None):
    return pl.pallas_call(
        kernel,
        name=name,
        out_shape=out_shape,
        in_specs=([] if scalars is None else [SMEM]) + [VMEM] * len(args),
        out_specs=jax.tree.map(lambda _: VMEM, out_shape),
        scratch_shapes=[pltpu.VMEM(s.shape, s.dtype) for s in scratch],
        compiler_params=pltpu.CompilerParams(vmem_limit_bytes=VMEM_LIMIT),
    )(*([] if scalars is None else [scalars]), *args)


def on_device(rows, cols, history):
    route = Route(rows, cols)
    terms, norb, width = history.shape
    total = width * rows * cols
    half = norb // 2
    core = lax.axis_index("row") & 1

    levels = route.levels
    scatter = min(levels, (half // 8).bit_length() - 1)
    blocks = 1 << scatter
    where_m = jnp.stack([core, route.place(core, scatter)])
    parts_levels = route.row_levels
    parts = 1 << parts_levels
    where_g = jnp.stack([core, route.place(core, parts_levels), route.place(1 - core, parts_levels)])

    own = [history[j] for j in range(terms)]
    peer = [swap(h, route.core_perm()) for h in own]
    left = call(
        functools.partial(arrange_kernel, blocks),
        "arrange",
        jax.ShapeDtypeStruct((half, 12 * width), jnp.bfloat16),
        [f32(half, 2 * width)],
        [own[0], peer[0]],
        where_m,
    )
    m = []
    for j in range(terms):
        keep, send = call(project_kernel, "project", [f32(half // 2, norb)] * 2, [], [left, own[j], peer[j]])
        m.append(all_reduce(route, keep, send, scatter, levels))
    mine = []
    for j in range(terms):
        scale = WEIGHTS[j] / total
        mine = [call(functools.partial(predict_kernel, scale), "predict", f32(half, 2 * width), [], [m[j], own[j], peer[j]] + mine)]
    mine = call(functools.partial(restore_kernel, blocks), "restore", f32(half, 2 * width), [], mine, where_m)
    other = swap(mine, route.core_perm())

    shares = (norb // TILE) * (norb // TILE + 1) // 2
    share = (shares + 1) // 2 * TILE
    ways = 1 << min(2, parts_levels)
    *pieces, predicted = call(
        functools.partial(gram_kernel, parts, 1.0 / total),
        "gram",
        [f32(share // ways, TILE)] * ways + [f32(norb, width)],
        [f32(norb, 2 * width), f32(share, TILE)],
        [mine, other],
        where_g,
    )
    gram = direct_all_reduce(route, pieces, parts_levels, levels)
    gram_other = swap(gram, route.core_perm())
    return call(
        functools.partial(solve_kernel, parts),
        "solve",
        f32(norb, width),
        [
            f32(2, share, TILE),
            f32(norb, norb + width),
            jax.ShapeDtypeStruct((6 * TILE, norb), jnp.bfloat16),
            jax.ShapeDtypeStruct((6 * TILE, norb + width), jnp.bfloat16),
        ],
        [gram, gram_other, predicted],
        where_g,
    )


def solution(mesh):
    return jax.shard_map(
        functools.partial(on_device, mesh.shape["row"], mesh.shape["col"]),
        mesh=mesh,
        in_specs=(P(None, None, ("row", "col")),),
        out_specs=P(None, ("row", "col")),
        check_vma=False,
    )
```

```python
import functools

import jax
import jax.numpy as jnp
from jax import lax
from jax.experimental import pallas as pl
from jax.experimental.pallas import tpu as pltpu
from jax.sharding import PartitionSpec as P

HIGHEST = lax.Precision.HIGHEST
WEIGHTS = (2.5, -2.0, 0.5)
TILE = 128
PANEL = 32
GROUP = 16
CHUNKS = 2
VMEM_LIMIT = 16 << 20
AXES = ("row", "col")
NT = (((1,), (1,)), ((), ()))
NN = (((1,), (0,)), ((), ()))
TN = (((0,), (0,)), ((), ()))


def dot(a, b, dims):
    return lax.dot_general(a, b, dims, precision=HIGHEST, preferred_element_type=jnp.float32)


def bf16_dot(a, b, dims):
    return lax.dot_general(a, b, dims, preferred_element_type=jnp.float32)


def split(x):
    high = x.astype(jnp.bfloat16)
    rest = x - high.astype(jnp.float32)
    middle = rest.astype(jnp.bfloat16)
    return high, middle, (rest - middle.astype(jnp.float32)).astype(jnp.bfloat16)


def stacked(x, axis):
    h, m, low = split(x)
    return jnp.concatenate([h, h, m, h, low, m], axis=axis), jnp.concatenate([h, m, h, low, h, m], axis=axis)


class Route:
    def __init__(self, mesh_rows, mesh_cols):
        self.rows, self.cols = mesh_rows, mesh_cols
        row_bits = list(range(1, mesh_rows.bit_length() - 1))
        col_bits = list(range(mesh_cols.bit_length() - 1))
        half = len(row_bits) // 2
        orders = (row_bits, row_bits[half:] + row_bits[:half])
        self.row_levels = len(row_bits)
        self.orders = tuple(
            [("row", b) for b in order] + [("col", b) for b in col_bits] for order in orders
        )
        self.levels = len(self.orders[0])

    def core_perm(self):
        c = self.cols
        return [(r * c + k, (r ^ 1) * c + k) for r in range(self.rows) for k in range(c)]

    def perm(self, *levels):
        pairs = []
        for r in range(self.rows):
            for k in range(self.cols):
                flip = {"row": 0, "col": 0}
                for level in levels:
                    axis, bit = self.orders[r & 1][level]
                    flip[axis] ^= 1 << bit
                pairs.append((r * self.cols + k, (r ^ flip["row"]) * self.cols + (k ^ flip["col"])))
        return pairs

    def perms(self, first, count):
        return [
            self.perm(*[first + i for i in range(count) if q >> (count - 1 - i) & 1]) for q in range(1, 1 << count)
        ]

    def place(self, core, levels):
        index = {"row": lax.axis_index("row"), "col": lax.axis_index("col")}
        numbers = []
        for order in self.orders:
            number = jnp.int32(0)
            for axis, bit in order[:levels]:
                number = number * 2 + ((index[axis] >> bit) & 1)
            numbers.append(number)
        return jnp.where(core == 0, numbers[0], numbers[1])


def swap(x, perm):
    return lax.ppermute(x, AXES, perm)


def all_reduce(route, keep, send, scatter, levels):
    for level in range(scatter):
        got = swap(send, route.perm(level))
        if level < scatter - 1:
            half = keep.shape[0] // 2
            keep, send = keep[:half] + got[:half], keep[half:] + got[half:]
        else:
            keep = keep + got
    for level in range(scatter, levels):
        keep = keep + swap(keep, route.perm(level))
    for level in reversed(range(scatter)):
        keep = jnp.concatenate([keep, swap(keep, route.perm(level))], axis=0)
    return keep


def phases(first, last):
    return [(level, min(2, last - level)) for level in range(first, last, 2)]


def direct_all_reduce(route, pieces, scatter, levels):
    for number, (level, count) in enumerate(phases(0, scatter)):
        if number > 0:
            size = keep.shape[0] >> count
            pieces = [keep[q * size : (q + 1) * size] for q in range(1 << count)]
        got = [swap(piece, perm) for piece, perm in zip(pieces[1:], route.perms(level, count))]
        keep = functools.reduce(jnp.add, got, pieces[0])
    for level, count in phases(scatter, levels):
        keep = functools.reduce(jnp.add, [swap(keep, perm) for perm in route.perms(level, count)], keep)
    for level, count in reversed(phases(0, scatter)):
        keep = jnp.concatenate([keep] + [swap(keep, perm) for perm in route.perms(level, count)])
    return keep


def arrange_kernel(blocks, where, own_ref, peer_ref, out_ref, left):
    rows, width = left.shape[0], own_ref.shape[1]
    core, place = where[0], where[1]
    size = rows // blocks
    for k in range(blocks):
        at = pl.multiple_of(core * rows + (place ^ k) * size, size)
        left[k * size : (k + 1) * size, :width] = own_ref[pl.ds(at, size), :]
        left[k * size : (k + 1) * size, width:] = peer_ref[pl.ds(at, size), :]
    out_ref[...] = stacked(left[...], axis=1)[0]


def project_kernel(pieces, left_ref, *refs):
    ins, (keep_ref, send_ref) = refs[:-2], refs[-2:]
    half, at = keep_ref.shape[0], 0
    for n, (low, high) in enumerate(pieces):
        x = jnp.concatenate([ins[2 * n][low:high, :], ins[2 * n + 1][low:high, :]], axis=1)
        right = stacked(x, axis=1)[1]
        keep_ref[:, at : at + high - low] = bf16_dot(left_ref[:half, :], right, NT)
        send_ref[:, at : at + high - low] = bf16_dot(left_ref[half:, :], right, NT)
        at += high - low


def predict_kernel(pieces, scales, m_ref, *refs):
    out_ref, at = refs[-1], 0
    for n, (low, high) in enumerate(pieces):
        x = jnp.concatenate([refs[2 * n][low:high, :], refs[2 * n + 1][low:high, :]], axis=1)
        left, right = stacked(m_ref[:, at : at + high - low], axis=1)[0], stacked(x, axis=0)[1]
        term = bf16_dot(left, right, NN) * scales[n]
        total = term if n == 0 else total + term
        at += high - low
    out_ref[...] = total + refs[2 * len(pieces)][...] if len(refs) > 2 * len(pieces) + 1 else total


def chunked(terms, rows, chunks):
    edges = [terms * rows * c // chunks // TILE * TILE for c in range(chunks)] + [terms * rows]
    result = []
    for first, last in zip(edges, edges[1:]):
        inside = [(j, max(first - j * rows, 0), min(last - j * rows, rows)) for j in range(terms)]
        result.append([piece for piece in inside if piece[1] < piece[2]])
    return result


def core_blocks(count):
    blocks = [(i, j) for i in range(count) for j in range(i, count)]
    half = (len(blocks) + 1) // 2
    return blocks[:half], blocks[half:]


def restore_kernel(blocks, where, in_ref, out_ref):
    size = in_ref.shape[0] // blocks
    for k in range(blocks):
        out_ref[pl.ds(pl.multiple_of((where[1] ^ k) * size, size), size), :] = in_ref[k * size : (k + 1) * size, :]


def gram_kernel(parts, scale, where, mine_ref, other_ref, *refs):
    outs, own_ref, p, acc = refs[:-3], refs[-3], refs[-2], refs[-1]
    half, width = mine_ref.shape[0], own_ref.shape[1]
    count = 2 * half // TILE
    lists = core_blocks(count)
    core, place = where[0], where[1]
    here = pl.ds(pl.multiple_of(core * half, half), half)
    there = pl.ds(pl.multiple_of((1 - core) * half, half), half)
    p[here, :] = mine_ref[...]
    p[there, :width] = other_ref[:, width:]
    p[there, width:] = other_ref[:, :width]
    own_ref[...] = p[:, :width]
    for n in range(len(lists[0])):
        first = lists[0][n]
        second = lists[1][min(n, len(lists[1]) - 1)]
        i = jnp.where(core == 0, first[0], second[0])
        j = jnp.where(core == 0, first[1], second[1])
        a = p[pl.ds(pl.multiple_of(i * TILE, TILE), TILE), :]
        b = p[pl.ds(pl.multiple_of(j * TILE, TILE), TILE), :]
        acc[n * TILE : (n + 1) * TILE, :] = dot(a, b, NT) * scale
    size = acc.shape[0] // parts
    for k in range(parts):
        each = parts // len(outs)
        outs[k // each][k % each * size : (k % each + 1) * size, :] = acc[pl.ds(pl.multiple_of((place ^ k) * size, 8), size), :]


def solve_kernel(parts, where, mine_ref, other_ref, p_ref, out_ref, natural, work, stack_a, stack_b):
    n, tile = p_ref.shape[0], TILE
    width = n + p_ref.shape[1]
    count, groups, per_panel, panels = n // tile, width // tile, PANEL // 8, tile // PANEL
    core, size = where[0], mine_ref.shape[0] // parts
    for ref, number, place in ((mine_ref, core, where[1]), (other_ref, 1 - core, where[2])):
        for k in range(parts):
            at = pl.multiple_of((place ^ k) * size, 8)
            natural[number, pl.ds(at, size), :] = ref[k * size : (k + 1) * size, :]
    for number, blocks in enumerate(core_blocks(count)):
        for at, (i, j) in enumerate(blocks):
            work[i * tile : (i + 1) * tile, j * tile : (j + 1) * tile] = natural[number, at * tile : (at + 1) * tile, :]
    work[:, n:] = p_ref[...]
    sub = lax.broadcasted_iota(jnp.int32, (8, tile), 0)
    deep = 6 * PANEL

    def panel(b, s):
        base = b * tile + PANEL * s
        r = [
            [work[base + 8 * i : base + 8 * i + 8, c * tile : (c + 1) * tile] for c in range(b, groups)]
            for i in range(per_panel)
        ]
        scale = [jnp.zeros((8, tile), jnp.float32)] * per_panel
        cols = {}
        for j in range(PANEL):
            if j % GROUP == 0:
                cols = {
                    k: {
                        i: jnp.broadcast_to(r[i][0][:, PANEL * s + k : PANEL * s + k + 1], (8, tile))
                        for i in range(k // 8, per_panel)
                    }
                    for k in range(j, j + GROUP)
                }
            jb, js = j // 8, j % 8
            col = cols[j]
            pivot = jnp.broadcast_to(col[jb][js : js + 1, :], (8, tile))
            scale[jb] = jnp.where(sub == js, lax.rsqrt(pivot), scale[jb])
            inverse = 1.0 / pivot
            mult = {i: col[i] * inverse for i in range(jb, per_panel)}
            mult[jb] = jnp.where(sub > js, mult[jb], 0.0)
            first = jb if js < 7 else jb + 1
            for k in range(j + 1, (j // GROUP + 1) * GROUP):
                row = jnp.broadcast_to(col[k // 8][k % 8 : k % 8 + 1, :], (8, tile))
                for i in range(k // 8, per_panel):
                    cols[k][i] = cols[k][i] - mult[i] * row
            for c in range(groups - b):
                row = jnp.broadcast_to(r[jb][c][js : js + 1, :], (8, tile))
                for i in range(first, per_panel):
                    r[i][c] = r[i][c] - mult[i] * row
        return jnp.concatenate(
            [jnp.concatenate([x * scale[i] for x in r[i]], axis=1) for i in range(per_panel)], axis=0
        )

    for b in range(count):
        start = b * tile
        for s in range(panels):
            u = panel(b, s)
            out_ref[start + PANEL * s : start + PANEL * (s + 1), :] = u[:, n - start :]
            if b == count - 1 and s == panels - 1:
                break
            left, right = stacked(u, axis=0)
            if s < panels - 1:
                low = PANEL * (s + 1)
                update = bf16_dot(left[:, :tile], right, TN)
                work[start + low : start + tile, start:] -= update[low:, :]
            if b < count - 1:
                stack_a[deep * s : deep * (s + 1), start:n] = left[:, : n - start]
                stack_b[deep * s : deep * (s + 1), start:] = right
        for i in range(b + 1, count):
            at = i * tile
            work[at : at + tile, at:] -= bf16_dot(stack_a[:, at : at + tile], stack_b[:, at:], TN)


VMEM = pl.BlockSpec(memory_space=pltpu.VMEM)
SMEM = pl.BlockSpec(memory_space=pltpu.SMEM)


def f32(*shape):
    return jax.ShapeDtypeStruct(shape, jnp.float32)


def call(kernel, name, out_shape, scratch, args, scalars=None):
    return pl.pallas_call(
        kernel,
        name=name,
        out_shape=out_shape,
        in_specs=([] if scalars is None else [SMEM]) + [VMEM] * len(args),
        out_specs=jax.tree.map(lambda _: VMEM, out_shape),
        scratch_shapes=[pltpu.VMEM(s.shape, s.dtype) for s in scratch],
        compiler_params=pltpu.CompilerParams(vmem_limit_bytes=VMEM_LIMIT),
    )(*([] if scalars is None else [scalars]), *args)


def on_device(rows, cols, history):
    route = Route(rows, cols)
    terms, norb, width = history.shape
    total = width * rows * cols
    half = norb // 2
    core = lax.axis_index("row") & 1

    levels = route.levels
    scatter = min(levels, (half // 8).bit_length() - 1)
    blocks = 1 << scatter
    where_m = jnp.stack([core, route.place(core, scatter)])
    parts_levels = route.row_levels
    parts = 1 << parts_levels
    where_g = jnp.stack([core, route.place(core, parts_levels), route.place(1 - core, parts_levels)])

    own = [history[j] for j in range(terms)]
    peer = [swap(h, route.core_perm()) for h in own]
    left = call(
        functools.partial(arrange_kernel, blocks),
        "arrange",
        jax.ShapeDtypeStruct((half, 12 * width), jnp.bfloat16),
        [f32(half, 2 * width)],
        [own[0], peer[0]],
        where_m,
    )
    chunks = chunked(terms, norb, CHUNKS)
    m, mine = [], []
    for chunk in chunks:
        rows_of = tuple(piece[1:] for piece in chunk)
        sides = [x for piece in chunk for x in (own[piece[0]], peer[piece[0]])]
        columns = sum(high - low for low, high in rows_of)
        keep, send = call(
            functools.partial(project_kernel, rows_of), "project", [f32(half // 2, columns)] * 2, [], [left] + sides
        )
        m.append(all_reduce(route, keep, send, scatter, levels))
    for chunk, product in zip(chunks, m):
        rows_of = tuple(piece[1:] for piece in chunk)
        sides = [x for piece in chunk for x in (own[piece[0]], peer[piece[0]])]
        scales = tuple(WEIGHTS[piece[0]] / total for piece in chunk)
        mine = [
            call(
                functools.partial(predict_kernel, rows_of, scales),
                "predict",
                f32(half, 2 * width),
                [],
                [product] + sides + mine,
            )
        ]
    mine = call(functools.partial(restore_kernel, blocks), "restore", f32(half, 2 * width), [], mine, where_m)
    other = swap(mine, route.core_perm())

    shares = (norb // TILE) * (norb // TILE + 1) // 2
    share = (shares + 1) // 2 * TILE
    ways = 1 << min(2, parts_levels)
    *pieces, predicted = call(
        functools.partial(gram_kernel, parts, 1.0 / total),
        "gram",
        [f32(share // ways, TILE)] * ways + [f32(norb, width)],
        [f32(norb, 2 * width), f32(share, TILE)],
        [mine, other],
        where_g,
    )
    gram = direct_all_reduce(route, pieces, parts_levels, levels)
    gram_other = swap(gram, route.core_perm())
    return call(
        functools.partial(solve_kernel, parts),
        "solve",
        f32(norb, width),
        [
            f32(2, share, TILE),
            f32(norb, norb + width),
            jax.ShapeDtypeStruct((6 * TILE, norb), jnp.bfloat16),
            jax.ShapeDtypeStruct((6 * TILE, norb + width), jnp.bfloat16),
        ],
        [gram, gram_other, predicted],
        where_g,
    )


def solution(mesh):
    return jax.shard_map(
        functools.partial(on_device, mesh.shape["row"], mesh.shape["col"]),
        mesh=mesh,
        in_specs=(P(None, None, ("row", "col")),),
        out_specs=P(None, ("row", "col")),
        check_vma=False,
    )
```

```python
import functools

import jax
import jax.numpy as jnp
from jax import lax
from jax.experimental import pallas as pl
from jax.experimental.pallas import tpu as pltpu
from jax.sharding import PartitionSpec as P

HIGHEST = lax.Precision.HIGHEST
WEIGHTS = (2.5, -2.0, 0.5)
TILE = 128
PANEL = 32
GROUP = 16
AHEAD = 4
VMEM_LIMIT = 16 << 20
AXES = ("row", "col")
NT = (((1,), (1,)), ((), ()))
NN = (((1,), (0,)), ((), ()))
TN = (((0,), (0,)), ((), ()))


def dot(a, b, dims):
    return lax.dot_general(a, b, dims, precision=HIGHEST, preferred_element_type=jnp.float32)


def bf16_dot(a, b, dims):
    return lax.dot_general(a, b, dims, preferred_element_type=jnp.float32)


def split(x):
    high = x.astype(jnp.bfloat16)
    rest = x - high.astype(jnp.float32)
    middle = rest.astype(jnp.bfloat16)
    return high, middle, (rest - middle.astype(jnp.float32)).astype(jnp.bfloat16)


def stacked(x, axis):
    h, m, low = split(x)
    return jnp.concatenate([h, h, m, h, low, m], axis=axis), jnp.concatenate([h, m, h, low, h, m], axis=axis)


class Route:
    def __init__(self, mesh_rows, mesh_cols):
        self.rows, self.cols = mesh_rows, mesh_cols
        row_bits = list(range(1, mesh_rows.bit_length() - 1))
        col_bits = list(range(mesh_cols.bit_length() - 1))
        half = len(row_bits) // 2
        orders = (row_bits, row_bits[half:] + row_bits[:half])
        self.row_levels = len(row_bits)
        self.orders = tuple(
            [("row", b) for b in order] + [("col", b) for b in col_bits] for order in orders
        )
        self.levels = len(self.orders[0])

    def core_perm(self):
        c = self.cols
        return [(r * c + k, (r ^ 1) * c + k) for r in range(self.rows) for k in range(c)]

    def perm(self, *levels):
        pairs = []
        for r in range(self.rows):
            for k in range(self.cols):
                flip = {"row": 0, "col": 0}
                for level in levels:
                    axis, bit = self.orders[r & 1][level]
                    flip[axis] ^= 1 << bit
                pairs.append((r * self.cols + k, (r ^ flip["row"]) * self.cols + (k ^ flip["col"])))
        return pairs

    def perms(self, first, count):
        return [
            self.perm(*[first + i for i in range(count) if q >> (count - 1 - i) & 1]) for q in range(1, 1 << count)
        ]

    def place(self, core, levels):
        index = {"row": lax.axis_index("row"), "col": lax.axis_index("col")}
        numbers = []
        for order in self.orders:
            number = jnp.int32(0)
            for axis, bit in order[:levels]:
                number = number * 2 + ((index[axis] >> bit) & 1)
            numbers.append(number)
        return jnp.where(core == 0, numbers[0], numbers[1])


def swap(x, perm):
    return lax.ppermute(x, AXES, perm)


def all_reduce(route, keep, send, scatter, levels):
    for level in range(scatter):
        got = swap(send, route.perm(level))
        if level < scatter - 1:
            half = keep.shape[0] // 2
            keep, send = keep[:half] + got[:half], keep[half:] + got[half:]
        else:
            keep = keep + got
    for level in range(scatter, levels):
        keep = keep + swap(keep, route.perm(level))
    for level in reversed(range(scatter)):
        keep = jnp.concatenate([keep, swap(keep, route.perm(level))], axis=0)
    return keep


def phases(first, last):
    return [(level, min(2, last - level)) for level in range(first, last, 2)]


def direct_all_reduce(route, pieces, scatter, levels):
    for number, (level, count) in enumerate(phases(0, scatter)):
        if number > 0:
            size = keep.shape[0] >> count
            pieces = [keep[q * size : (q + 1) * size] for q in range(1 << count)]
        got = [swap(piece, perm) for piece, perm in zip(pieces[1:], route.perms(level, count))]
        keep = functools.reduce(jnp.add, got, pieces[0])
    for level, count in phases(scatter, levels):
        keep = functools.reduce(jnp.add, [swap(keep, perm) for perm in route.perms(level, count)], keep)
    for level, count in reversed(phases(0, scatter)):
        keep = jnp.concatenate([keep] + [swap(keep, perm) for perm in route.perms(level, count)])
    return keep


def fetch_kernel(in_ref, out_ref):
    pltpu.sync_copy(in_ref, out_ref)


def project_kernel(j, left_ref, own_ref, peer_ref, keep_ref, send_ref):
    half = keep_ref.shape[0]
    right = stacked(jnp.concatenate([own_ref[j], peer_ref[j]], axis=1), axis=1)[1]
    keep_ref[...] = bf16_dot(left_ref[:half, :], right, NT)
    send_ref[...] = bf16_dot(left_ref[half:, :], right, NT)


def first_project_kernel(blocks, where, own_ref, peer_ref, keep_ref, send_ref, left_ref, left):
    rows, width = left.shape[0], own_ref.shape[2]
    core, place = where[0], where[1]
    size = rows // blocks
    for k in range(blocks):
        at = pl.multiple_of(core * rows + (place ^ k) * size, size)
        left[k * size : (k + 1) * size, :width] = own_ref[0, pl.ds(at, size), :]
        left[k * size : (k + 1) * size, width:] = peer_ref[0, pl.ds(at, size), :]
    left_ref[...] = stacked(left[...], axis=1)[0]
    project_kernel(0, left_ref, own_ref, peer_ref, keep_ref, send_ref)


def term(j, scale, m_ref, own_ref, peer_ref):
    left = stacked(m_ref[...], axis=1)[0]
    right = stacked(jnp.concatenate([own_ref[j], peer_ref[j]], axis=1), axis=0)[1]
    return bf16_dot(left, right, NN) * scale


def predict_kernel(j, scale, m_ref, own_ref, peer_ref, *refs):
    value = term(j, scale, m_ref, own_ref, peer_ref)
    refs[-1][...] = value + refs[0][...] if len(refs) > 1 else value


def last_predict_kernel(j, scale, blocks, where, m_ref, own_ref, peer_ref, sum_ref, out_ref, total):
    total[...] = term(j, scale, m_ref, own_ref, peer_ref) + sum_ref[...]
    size = total.shape[0] // blocks
    for k in range(blocks):
        out_ref[pl.ds(pl.multiple_of((where[1] ^ k) * size, size), size), :] = total[k * size : (k + 1) * size, :]


def core_blocks(count):
    blocks = [(i, j) for i in range(count) for j in range(i, count)]
    half = (len(blocks) + 1) // 2
    return blocks[:half], blocks[half:]


def gram_kernel(parts, scale, where, mine_ref, other_ref, *refs):
    outs, own_ref, p, acc = refs[:-3], refs[-3], refs[-2], refs[-1]
    half, width = mine_ref.shape[0], own_ref.shape[1]
    count = 2 * half // TILE
    lists = core_blocks(count)
    core, place = where[0], where[1]
    here = pl.ds(pl.multiple_of(core * half, half), half)
    there = pl.ds(pl.multiple_of((1 - core) * half, half), half)
    p[here, :] = mine_ref[...]
    p[there, :width] = other_ref[:, width:]
    p[there, width:] = other_ref[:, :width]
    own_ref[...] = p[:, :width]
    for n in range(len(lists[0])):
        first = lists[0][n]
        second = lists[1][min(n, len(lists[1]) - 1)]
        i = jnp.where(core == 0, first[0], second[0])
        j = jnp.where(core == 0, first[1], second[1])
        a = p[pl.ds(pl.multiple_of(i * TILE, TILE), TILE), :]
        b = p[pl.ds(pl.multiple_of(j * TILE, TILE), TILE), :]
        acc[n * TILE : (n + 1) * TILE, :] = dot(a, b, NT) * scale
    size = acc.shape[0] // parts
    for k in range(parts):
        each = parts // len(outs)
        outs[k // each][k % each * size : (k % each + 1) * size, :] = acc[pl.ds(pl.multiple_of((place ^ k) * size, 8), size), :]


def solve_kernel(parts, where, mine_ref, other_ref, p_ref, out_ref, natural, work, stack_a, stack_b):
    n, tile = p_ref.shape[0], TILE
    width = n + p_ref.shape[1]
    count, groups, per_panel, panels = n // tile, width // tile, PANEL // 8, tile // PANEL
    core, size = where[0], mine_ref.shape[0] // parts
    for ref, number, place in ((mine_ref, core, where[1]), (other_ref, 1 - core, where[2])):
        for k in range(parts):
            at = pl.multiple_of((place ^ k) * size, 8)
            natural[number, pl.ds(at, size), :] = ref[k * size : (k + 1) * size, :]
    for number, blocks in enumerate(core_blocks(count)):
        for at, (i, j) in enumerate(blocks):
            work[i * tile : (i + 1) * tile, j * tile : (j + 1) * tile] = natural[number, at * tile : (at + 1) * tile, :]
    work[:, n:] = p_ref[...]
    sub = lax.broadcasted_iota(jnp.int32, (8, tile), 0)
    deep = 6 * PANEL

    def panel(b, s):
        base = b * tile + PANEL * s
        r = [
            [work[base + 8 * i : base + 8 * i + 8, c * tile : (c + 1) * tile] for c in range(b, groups)]
            for i in range(per_panel)
        ]
        scale = [jnp.zeros((8, tile), jnp.float32)] * per_panel
        cols = {}
        for j in range(PANEL):
            start = 0 if j == 0 else j + AHEAD
            if start % GROUP == 0 and start < PANEL:
                for k in range(start, start + GROUP):
                    at = PANEL * s + k
                    cols[k] = {i: jnp.broadcast_to(r[i][0][:, at : at + 1], (8, tile)) for i in range(k // 8, per_panel)}
            jb, js = j // 8, j % 8
            col = cols[j]
            pivot = jnp.broadcast_to(col[jb][js : js + 1, :], (8, tile))
            scale[jb] = jnp.where(sub == js, lax.rsqrt(pivot), scale[jb])
            inverse = 1.0 / pivot
            mult = {i: col[i] * inverse for i in range(jb, per_panel)}
            mult[jb] = jnp.where(sub > js, mult[jb], 0.0)
            first = jb if js < 7 else jb + 1
            for k in range(j + 1, len(cols)):
                row = jnp.broadcast_to(col[k // 8][k % 8 : k % 8 + 1, :], (8, tile))
                for i in range(k // 8, per_panel):
                    cols[k][i] = cols[k][i] - mult[i] * row
            for c in range(groups - b):
                row = jnp.broadcast_to(r[jb][c][js : js + 1, :], (8, tile))
                for i in range(first, per_panel):
                    r[i][c] = r[i][c] - mult[i] * row
        return jnp.concatenate(
            [jnp.concatenate([x * scale[i] for x in r[i]], axis=1) for i in range(per_panel)], axis=0
        )

    for b in range(count):
        start = b * tile
        for s in range(panels):
            u = panel(b, s)
            out_ref[start + PANEL * s : start + PANEL * (s + 1), :] = u[:, n - start :]
            if b == count - 1 and s == panels - 1:
                break
            left, right = stacked(u, axis=0)
            if s < panels - 1:
                flipped = jnp.transpose(left[:, :tile])
                low, high, near = PANEL * (s + 1), PANEL * (s + 2), min(start + 2 * tile, width)
                for rows, columns in (((low, high), (start, near)), ((low, high), (near, width)), ((high, tile), (start, width))):
                    if rows[0] < rows[1] and columns[0] < columns[1]:
                        work[start + rows[0] : start + rows[1], columns[0] : columns[1]] -= bf16_dot(
                            flipped[rows[0] : rows[1], :], right[:, columns[0] - start : columns[1] - start], NN
                        )
            if b < count - 1:
                stack_a[deep * s : deep * (s + 1), start:n] = left[:, : n - start]
                stack_b[deep * s : deep * (s + 1), start:] = right
        for i in range(b + 1, count):
            at = i * tile
            work[at : at + tile, at:] -= bf16_dot(stack_a[:, at : at + tile], stack_b[:, at:], TN)


VMEM = pl.BlockSpec(memory_space=pltpu.VMEM)
SMEM = pl.BlockSpec(memory_space=pltpu.SMEM)


def f32(*shape):
    return jax.ShapeDtypeStruct(shape, jnp.float32)


def call(kernel, name, out_shape, scratch, args, scalars=None):
    return pl.pallas_call(
        kernel,
        name=name,
        out_shape=out_shape,
        in_specs=([] if scalars is None else [SMEM]) + [VMEM] * len(args),
        out_specs=jax.tree.map(lambda _: VMEM, out_shape),
        scratch_shapes=[pltpu.VMEM(s.shape, s.dtype) for s in scratch],
        compiler_params=pltpu.CompilerParams(vmem_limit_bytes=VMEM_LIMIT),
    )(*([] if scalars is None else [scalars]), *args)


def on_device(rows, cols, history):
    route = Route(rows, cols)
    terms, norb, width = history.shape
    total = width * rows * cols
    half = norb // 2
    core = lax.axis_index("row") & 1

    levels = route.levels
    scatter = min(levels, (half // 8).bit_length() - 1)
    blocks = 1 << scatter
    where_m = jnp.stack([core, route.place(core, scatter)])
    parts_levels = route.row_levels
    parts = 1 << parts_levels
    where_g = jnp.stack([core, route.place(core, parts_levels), route.place(1 - core, parts_levels)])

    peer = swap(history, route.core_perm())
    own = pl.pallas_call(
        fetch_kernel,
        name="fetch",
        out_shape=f32(*history.shape),
        in_specs=[pl.BlockSpec(memory_space=pl.ANY)],
        out_specs=VMEM,
        compiler_params=pltpu.CompilerParams(vmem_limit_bytes=VMEM_LIMIT),
    )(history)
    out = [f32(half // 2, norb)] * 2
    keep, send, left = call(
        functools.partial(first_project_kernel, blocks),
        "project",
        out + [jax.ShapeDtypeStruct((half, 12 * width), jnp.bfloat16)],
        [f32(half, 2 * width)],
        [own, peer],
        where_m,
    )
    products = [(keep, send)]
    for j in range(1, terms):
        products.append(call(functools.partial(project_kernel, j), "project", out, [], [left, own, peer]))
    m = [all_reduce(route, keep, send, scatter, levels) for keep, send in products]
    out, mine = f32(half, 2 * width), []
    for j in range(terms - 1):
        kernel = functools.partial(predict_kernel, j, WEIGHTS[j] / total)
        mine = [call(kernel, "predict", out, [], [m[j], own, peer] + mine)]
    kernel = functools.partial(last_predict_kernel, terms - 1, WEIGHTS[terms - 1] / total, blocks)
    mine = call(kernel, "predict", out, [out], [m[-1], own, peer] + mine, where_m)
    other = swap(mine, route.core_perm())

    shares = (norb // TILE) * (norb // TILE + 1) // 2
    share = (shares + 1) // 2 * TILE
    ways = 1 << min(2, parts_levels)
    *pieces, predicted = call(
        functools.partial(gram_kernel, parts, 1.0 / total),
        "gram",
        [f32(share // ways, TILE)] * ways + [f32(norb, width)],
        [f32(norb, 2 * width), f32(share, TILE)],
        [mine, other],
        where_g,
    )
    gram = direct_all_reduce(route, pieces, parts_levels, levels)
    gram_other = swap(gram, route.core_perm())
    return call(
        functools.partial(solve_kernel, parts),
        "solve",
        f32(norb, width),
        [
            f32(2, share, TILE),
            f32(norb, norb + width),
            jax.ShapeDtypeStruct((6 * TILE, norb), jnp.bfloat16),
            jax.ShapeDtypeStruct((6 * TILE, norb + width), jnp.bfloat16),
        ],
        [gram, gram_other, predicted],
        where_g,
    )


def solution(mesh):
    return jax.shard_map(
        functools.partial(on_device, mesh.shape["row"], mesh.shape["col"]),
        mesh=mesh,
        in_specs=(P(None, None, ("row", "col")),),
        out_specs=P(None, ("row", "col")),
        check_vma=False,
    )
```

```python
import functools

import jax
import jax.numpy as jnp
from jax import lax
from jax.experimental import pallas as pl
from jax.experimental.pallas import tpu as pltpu
from jax.sharding import PartitionSpec as P

HIGHEST = lax.Precision.HIGHEST
WEIGHTS = (2.5, -2.0, 0.5)
TILE = 128
PANEL = 32
GROUP = 16
AHEAD = 4
VMEM_LIMIT = 16 << 20
AXES = ("row", "col")
NT = (((1,), (1,)), ((), ()))
NN = (((1,), (0,)), ((), ()))
TN = (((0,), (0,)), ((), ()))


def dot(a, b, dims):
    return lax.dot_general(a, b, dims, precision=HIGHEST, preferred_element_type=jnp.float32)


def bf16_dot(a, b, dims):
    return lax.dot_general(a, b, dims, preferred_element_type=jnp.float32)


def split(x):
    high = x.astype(jnp.bfloat16)
    rest = x - high.astype(jnp.float32)
    middle = rest.astype(jnp.bfloat16)
    return high, middle, (rest - middle.astype(jnp.float32)).astype(jnp.bfloat16)


def stacked(x, axis):
    h, m, low = split(x)
    return jnp.concatenate([h, h, m, h, low, m], axis=axis), jnp.concatenate([h, m, h, low, h, m], axis=axis)


class Route:
    def __init__(self, mesh_rows, mesh_cols):
        self.rows, self.cols = mesh_rows, mesh_cols
        row_bits = list(range(1, mesh_rows.bit_length() - 1))
        col_bits = list(range(mesh_cols.bit_length() - 1))
        half = len(row_bits) // 2
        orders = (row_bits, row_bits[half:] + row_bits[:half])
        self.row_levels = len(row_bits)
        self.orders = tuple(
            [("row", b) for b in order] + [("col", b) for b in col_bits] for order in orders
        )
        self.levels = len(self.orders[0])

    def core(self):
        return lax.axis_index("row") & 1

    def core_perm(self):
        c = self.cols
        return [(r * c + k, (r ^ 1) * c + k) for r in range(self.rows) for k in range(c)]

    def perm(self, *levels):
        pairs = []
        for r in range(self.rows):
            for k in range(self.cols):
                flip = {"row": 0, "col": 0}
                for level in levels:
                    axis, bit = self.orders[r & 1][level]
                    flip[axis] ^= 1 << bit
                pairs.append((r * self.cols + k, (r ^ flip["row"]) * self.cols + (k ^ flip["col"])))
        return pairs

    def perms(self, first, count):
        return [
            self.perm(*[first + i for i in range(count) if q >> (count - 1 - i) & 1]) for q in range(1, 1 << count)
        ]

    def place(self, core, levels):
        index = {"row": lax.axis_index("row"), "col": lax.axis_index("col")}
        numbers = []
        for order in self.orders:
            number = jnp.int32(0)
            for axis, bit in order[:levels]:
                number = number * 2 + ((index[axis] >> bit) & 1)
            numbers.append(number)
        return jnp.where(core == 0, numbers[0], numbers[1])


def swap(x, perm):
    return lax.ppermute(x, AXES, perm)


def all_reduce(route, keep, send, scatter, levels):
    for level in range(scatter):
        got = swap(send, route.perm(level))
        if level < scatter - 1:
            half = keep.shape[0] // 2
            keep, send = keep[:half] + got[:half], keep[half:] + got[half:]
        else:
            keep = keep + got
    for level in range(scatter, levels):
        keep = keep + swap(keep, route.perm(level))
    for level in reversed(range(scatter)):
        keep = jnp.concatenate([keep, swap(keep, route.perm(level))], axis=0)
    return keep


def phases(first, last):
    return [(level, min(2, last - level)) for level in range(first, last, 2)]


def direct_all_reduce(route, pieces, scatter, levels):
    for number, (level, count) in enumerate(phases(0, scatter)):
        if number > 0:
            size = keep.shape[0] >> count
            pieces = [keep[q * size : (q + 1) * size] for q in range(1 << count)]
        got = [swap(piece, perm) for piece, perm in zip(pieces[1:], route.perms(level, count))]
        keep = functools.reduce(jnp.add, got, pieces[0])
    for level, count in phases(scatter, levels):
        keep = functools.reduce(jnp.add, [swap(keep, perm) for perm in route.perms(level, count)], keep)
    for level, count in reversed(phases(0, scatter)):
        keep = jnp.concatenate([keep] + [swap(keep, perm) for perm in route.perms(level, count)])
    return keep


def fetch_kernel(in_ref, out_ref):
    pltpu.sync_copy(in_ref, out_ref)


def project_kernel(j, left_ref, own_ref, peer_ref, keep_ref, send_ref):
    half = keep_ref.shape[0]
    right = stacked(jnp.concatenate([own_ref[j], peer_ref[j]], axis=1), axis=1)[1]
    keep_ref[...] = bf16_dot(left_ref[:half, :], right, NT)
    send_ref[...] = bf16_dot(left_ref[half:, :], right, NT)


def first_project_kernel(route, scatter, own_ref, peer_ref, keep_ref, send_ref, left_ref, left):
    rows, width, blocks = left.shape[0], own_ref.shape[2], 1 << scatter
    core = route.core()
    place = route.place(core, scatter)
    size = rows // blocks
    for k in range(blocks):
        at = pl.multiple_of(core * rows + (place ^ k) * size, size)
        left[k * size : (k + 1) * size, :width] = own_ref[0, pl.ds(at, size), :]
        left[k * size : (k + 1) * size, width:] = peer_ref[0, pl.ds(at, size), :]
    left_ref[...] = stacked(left[...], axis=1)[0]
    project_kernel(0, left_ref, own_ref, peer_ref, keep_ref, send_ref)


def term(j, scale, m_ref, own_ref, peer_ref):
    left = stacked(m_ref[...], axis=1)[0]
    right = stacked(jnp.concatenate([own_ref[j], peer_ref[j]], axis=1), axis=0)[1]
    return bf16_dot(left, right, NN) * scale


def predict_kernel(j, scale, m_ref, own_ref, peer_ref, *refs):
    value = term(j, scale, m_ref, own_ref, peer_ref)
    refs[-1][...] = value + refs[0][...] if len(refs) > 1 else value


def last_predict_kernel(j, scale, route, scatter, m_ref, own_ref, peer_ref, sum_ref, out_ref, total):
    total[...] = term(j, scale, m_ref, own_ref, peer_ref) + sum_ref[...]
    place, blocks = route.place(route.core(), scatter), 1 << scatter
    size = total.shape[0] // blocks
    for k in range(blocks):
        out_ref[pl.ds(pl.multiple_of((place ^ k) * size, size), size), :] = total[k * size : (k + 1) * size, :]


def core_blocks(count):
    blocks = [(i, j) for i in range(count) for j in range(i, count)]
    half = (len(blocks) + 1) // 2
    return blocks[:half], blocks[half:]


def gram_kernel(route, scale, mine_ref, other_ref, *refs):
    outs, own_ref, p, acc = refs[:-3], refs[-3], refs[-2], refs[-1]
    half, width = mine_ref.shape[0], own_ref.shape[1]
    count = 2 * half // TILE
    lists = core_blocks(count)
    parts, core = 1 << route.row_levels, route.core()
    place = route.place(core, route.row_levels)
    here = pl.ds(pl.multiple_of(core * half, half), half)
    there = pl.ds(pl.multiple_of((1 - core) * half, half), half)
    p[here, :] = mine_ref[...]
    p[there, :width] = other_ref[:, width:]
    p[there, width:] = other_ref[:, :width]
    own_ref[...] = p[:, :width]
    for n in range(len(lists[0])):
        first = lists[0][n]
        second = lists[1][min(n, len(lists[1]) - 1)]
        i = jnp.where(core == 0, first[0], second[0])
        j = jnp.where(core == 0, first[1], second[1])
        a = p[pl.ds(pl.multiple_of(i * TILE, TILE), TILE), :]
        b = p[pl.ds(pl.multiple_of(j * TILE, TILE), TILE), :]
        acc[n * TILE : (n + 1) * TILE, :] = dot(a, b, NT) * scale
    size = acc.shape[0] // parts
    for k in range(parts):
        each = parts // len(outs)
        outs[k // each][k % each * size : (k % each + 1) * size, :] = acc[pl.ds(pl.multiple_of((place ^ k) * size, 8), size), :]


def solve_kernel(route, mine_ref, other_ref, p_ref, out_ref, natural, work, stack_a, stack_b):
    n, tile = p_ref.shape[0], TILE
    width = n + p_ref.shape[1]
    count, groups, per_panel, panels = n // tile, width // tile, PANEL // 8, tile // PANEL
    parts, core = 1 << route.row_levels, route.core()
    size = mine_ref.shape[0] // parts
    for ref, number in ((mine_ref, core), (other_ref, 1 - core)):
        place = route.place(number, route.row_levels)
        for k in range(parts):
            at = pl.multiple_of((place ^ k) * size, 8)
            natural[number, pl.ds(at, size), :] = ref[k * size : (k + 1) * size, :]
    for number, blocks in enumerate(core_blocks(count)):
        for at, (i, j) in enumerate(blocks):
            work[i * tile : (i + 1) * tile, j * tile : (j + 1) * tile] = natural[number, at * tile : (at + 1) * tile, :]
    work[:, n:] = p_ref[...]
    sub = lax.broadcasted_iota(jnp.int32, (8, tile), 0)
    deep = 6 * PANEL

    def panel(b, s):
        base = b * tile + PANEL * s
        r = [
            [work[base + 8 * i : base + 8 * i + 8, c * tile : (c + 1) * tile] for c in range(b, groups)]
            for i in range(per_panel)
        ]
        scale = [jnp.zeros((8, tile), jnp.float32)] * per_panel
        cols = {}
        for j in range(PANEL):
            start = 0 if j == 0 else j + AHEAD
            if start % GROUP == 0 and start < PANEL:
                for k in range(start, start + GROUP):
                    at = PANEL * s + k
                    cols[k] = {i: jnp.broadcast_to(r[i][0][:, at : at + 1], (8, tile)) for i in range(k // 8, per_panel)}
            jb, js = j // 8, j % 8
            col = cols[j]
            pivot = jnp.broadcast_to(col[jb][js : js + 1, :], (8, tile))
            scale[jb] = jnp.where(sub == js, lax.rsqrt(pivot), scale[jb])
            inverse = 1.0 / pivot
            mult = {i: col[i] * inverse for i in range(jb, per_panel)}
            mult[jb] = jnp.where(sub > js, mult[jb], 0.0)
            first = jb if js < 7 else jb + 1
            for k in range(j + 1, len(cols)):
                row = jnp.broadcast_to(col[k // 8][k % 8 : k % 8 + 1, :], (8, tile))
                for i in range(k // 8, per_panel):
                    cols[k][i] = cols[k][i] - mult[i] * row
            for c in range(groups - b):
                row = jnp.broadcast_to(r[jb][c][js : js + 1, :], (8, tile))
                for i in range(first, per_panel):
                    r[i][c] = r[i][c] - mult[i] * row
        return jnp.concatenate(
            [jnp.concatenate([x * scale[i] for x in r[i]], axis=1) for i in range(per_panel)], axis=0
        )

    for b in range(count):
        start = b * tile
        for s in range(panels):
            u = panel(b, s)
            out_ref[start + PANEL * s : start + PANEL * (s + 1), :] = u[:, n - start :]
            if b == count - 1 and s == panels - 1:
                break
            left, right = stacked(u, axis=0)
            if s < panels - 1:
                flipped = jnp.transpose(left[:, :tile])
                low, high, near = PANEL * (s + 1), PANEL * (s + 2), min(start + 2 * tile, width)
                for rows, columns in (((low, high), (start, near)), ((low, high), (near, width)), ((high, tile), (start, width))):
                    if rows[0] < rows[1] and columns[0] < columns[1]:
                        work[start + rows[0] : start + rows[1], columns[0] : columns[1]] -= bf16_dot(
                            flipped[rows[0] : rows[1], :], right[:, columns[0] - start : columns[1] - start], NN
                        )
            if b < count - 1:
                stack_a[deep * s : deep * (s + 1), start:n] = left[:, : n - start]
                stack_b[deep * s : deep * (s + 1), start:] = right
        for i in range(b + 1, count):
            at = i * tile
            work[at : at + tile, at:] -= bf16_dot(stack_a[:, at : at + tile], stack_b[:, at:], TN)


VMEM = pl.BlockSpec(memory_space=pltpu.VMEM)


def f32(*shape):
    return jax.ShapeDtypeStruct(shape, jnp.float32)


def call(kernel, name, out_shape, scratch, args):
    return pl.pallas_call(
        kernel,
        name=name,
        out_shape=out_shape,
        in_specs=[VMEM] * len(args),
        out_specs=jax.tree.map(lambda _: VMEM, out_shape),
        scratch_shapes=[pltpu.VMEM(s.shape, s.dtype) for s in scratch],
        compiler_params=pltpu.CompilerParams(vmem_limit_bytes=VMEM_LIMIT),
    )(*args)


def on_device(rows, cols, history):
    route = Route(rows, cols)
    terms, norb, width = history.shape
    total = width * rows * cols
    half = norb // 2

    levels = route.levels
    scatter = min(levels, (half // 8).bit_length() - 1)

    peer = swap(history, route.core_perm())
    own = pl.pallas_call(
        fetch_kernel,
        name="fetch",
        out_shape=f32(*history.shape),
        in_specs=[pl.BlockSpec(memory_space=pl.ANY)],
        out_specs=VMEM,
        compiler_params=pltpu.CompilerParams(vmem_limit_bytes=VMEM_LIMIT),
    )(history)
    out = [f32(half // 2, norb)] * 2
    keep, send, left = call(
        functools.partial(first_project_kernel, route, scatter),
        "project",
        out + [jax.ShapeDtypeStruct((half, 12 * width), jnp.bfloat16)],
        [f32(half, 2 * width)],
        [own, peer],
    )
    products = [(keep, send)]
    for j in range(1, terms):
        products.append(call(functools.partial(project_kernel, j), "project", out, [], [left, own, peer]))
    m = [all_reduce(route, keep, send, scatter, levels) for keep, send in products]
    out, mine = f32(half, 2 * width), []
    for j in range(terms - 1):
        kernel = functools.partial(predict_kernel, j, WEIGHTS[j] / total)
        mine = [call(kernel, "predict", out, [], [m[j], own, peer] + mine)]
    kernel = functools.partial(last_predict_kernel, terms - 1, WEIGHTS[terms - 1] / total, route, scatter)
    mine = call(kernel, "predict", out, [out], [m[-1], own, peer] + mine)
    other = swap(mine, route.core_perm())

    shares = (norb // TILE) * (norb // TILE + 1) // 2
    share = (shares + 1) // 2 * TILE
    ways = 1 << min(2, route.row_levels)
    *pieces, predicted = call(
        functools.partial(gram_kernel, route, 1.0 / total),
        "gram",
        [f32(share // ways, TILE)] * ways + [f32(norb, width)],
        [f32(norb, 2 * width), f32(share, TILE)],
        [mine, other],
    )
    gram = direct_all_reduce(route, pieces, route.row_levels, levels)
    gram_other = swap(gram, route.core_perm())
    return call(
        functools.partial(solve_kernel, route),
        "solve",
        f32(norb, width),
        [
            f32(2, share, TILE),
            f32(norb, norb + width),
            jax.ShapeDtypeStruct((6 * TILE, norb), jnp.bfloat16),
            jax.ShapeDtypeStruct((6 * TILE, norb + width), jnp.bfloat16),
        ],
        [gram, gram_other, predicted],
    )


def solution(mesh):
    return jax.shard_map(
        functools.partial(on_device, mesh.shape["row"], mesh.shape["col"]),
        mesh=mesh,
        in_specs=(P(None, None, ("row", "col")),),
        out_specs=P(None, ("row", "col")),
        check_vma=False,
    )
```

```python
import functools

import jax
import jax.numpy as jnp
from jax import lax
from jax.experimental import pallas as pl
from jax.experimental.pallas import tpu as pltpu
from jax.sharding import PartitionSpec as P


HIGHEST = lax.Precision.HIGHEST
WEIGHTS = (2.5, -2.0, 0.5)
TILE = 128
PANEL = 32
GROUP = 16
AHEAD = 4
VMEM_LIMIT = 16 << 20
AXES = ("row", "col")
NT = (((1,), (1,)), ((), ()))
NN = (((1,), (0,)), ((), ()))
TN = (((0,), (0,)), ((), ()))


def dot(a, b, dims):
    return lax.dot_general(a, b, dims, precision=HIGHEST, preferred_element_type=jnp.float32)


def bf16_dot(a, b, dims):
    return lax.dot_general(a, b, dims, preferred_element_type=jnp.float32)


def split(x):
    high = x.astype(jnp.bfloat16)
    rest = x - high.astype(jnp.float32)
    middle = rest.astype(jnp.bfloat16)
    return high, middle, (rest - middle.astype(jnp.float32)).astype(jnp.bfloat16)


def stacked(x, axis):
    h, m, low = split(x)
    return jnp.concatenate([h, h, m, h, low, m], axis=axis), jnp.concatenate([h, m, h, low, h, m], axis=axis)


class Route:
    def __init__(self, mesh_rows, mesh_cols):
        self.rows, self.cols = mesh_rows, mesh_cols
        row_bits = list(range(1, mesh_rows.bit_length() - 1))
        col_bits = list(range(mesh_cols.bit_length() - 1))
        half = len(row_bits) // 2
        orders = (row_bits, row_bits[half:] + row_bits[:half])
        self.row_levels = len(row_bits)
        self.orders = tuple(
            [("row", b) for b in order] + [("col", b) for b in col_bits] for order in orders
        )
        self.levels = len(self.orders[0])

    def scatter(self, norb):
        return min(self.levels, (norb // 16).bit_length() - 1)

    def core(self):
        return lax.axis_index("row") & 1

    def core_perm(self):
        c = self.cols
        return [(r * c + k, (r ^ 1) * c + k) for r in range(self.rows) for k in range(c)]

    def perm(self, *levels):
        pairs = []
        for r in range(self.rows):
            for k in range(self.cols):
                flip = {"row": 0, "col": 0}
                for level in levels:
                    axis, bit = self.orders[r & 1][level]
                    flip[axis] ^= 1 << bit
                pairs.append((r * self.cols + k, (r ^ flip["row"]) * self.cols + (k ^ flip["col"])))
        return pairs

    def perms(self, first, count):
        return [
            self.perm(*[first + i for i in range(count) if q >> (count - 1 - i) & 1]) for q in range(1, 1 << count)
        ]

    def place(self, core, levels):
        index = {"row": lax.axis_index("row"), "col": lax.axis_index("col")}
        numbers = []
        for order in self.orders:
            number = jnp.int32(0)
            for axis, bit in order[:levels]:
                number = number * 2 + ((index[axis] >> bit) & 1)
            numbers.append(number)
        return jnp.where(core == 0, numbers[0], numbers[1])


def swap(x, perm):
    return lax.ppermute(x, AXES, perm)


def all_reduce(route, keep, send, scatter, levels):
    def step(x, level):
        return swap(x, route.perm(level))

    for level in range(scatter):
        got = step(send, level)
        if level < scatter - 1:
            half = keep.shape[0] // 2
            keep, send = keep[:half] + got[:half], keep[half:] + got[half:]
        else:
            keep = keep + got
    for level in range(scatter, levels):
        keep = keep + step(keep, level)
    for level in reversed(range(scatter)):
        keep = jnp.concatenate([keep, step(keep, level)], axis=0)
    return keep


def phases(first, last):
    return [(level, min(2, last - level)) for level in range(first, last, 2)]


def direct_all_reduce(route, pieces, scatter, levels):
    for number, (level, count) in enumerate(phases(0, scatter)):
        if number > 0:
            size = keep.shape[0] >> count
            pieces = [keep[q * size : (q + 1) * size] for q in range(1 << count)]
        got = [swap(piece, perm) for piece, perm in zip(pieces[1:], route.perms(level, count))]
        keep = functools.reduce(jnp.add, got, pieces[0])
    for level, count in phases(scatter, levels):
        keep = functools.reduce(jnp.add, [swap(keep, perm) for perm in route.perms(level, count)], keep)
    for level, count in reversed(phases(0, scatter)):
        keep = jnp.concatenate([keep] + [swap(keep, perm) for perm in route.perms(level, count)])
    return keep


def fetch_kernel(in_ref, out_ref):
    pltpu.sync_copy(in_ref, out_ref)


def project_kernel(j, left_ref, own_ref, peer_ref, keep_ref, send_ref):
    half = keep_ref.shape[0]
    right = stacked(jnp.concatenate([own_ref[j], peer_ref[j]], axis=1), axis=1)[1]
    keep_ref[...] = bf16_dot(left_ref[:half, :], right, NT)
    send_ref[...] = bf16_dot(left_ref[half:, :], right, NT)


def first_project_kernel(route, scatter, own_ref, peer_ref, keep_ref, send_ref, left_ref, left):
    rows, width, blocks = left.shape[0], own_ref.shape[2], 1 << scatter
    core = route.core()
    place = route.place(core, scatter)
    size = rows // blocks
    for k in range(blocks):
        at = pl.multiple_of(core * rows + (place ^ k) * size, size)
        left[k * size : (k + 1) * size, :width] = own_ref[0, pl.ds(at, size), :]
        left[k * size : (k + 1) * size, width:] = peer_ref[0, pl.ds(at, size), :]
    left_ref[...] = stacked(left[...], axis=1)[0]
    project_kernel(0, left_ref, own_ref, peer_ref, keep_ref, send_ref)


def term(j, scale, m_ref, own_ref, peer_ref):
    left = stacked(m_ref[...], axis=1)[0]
    right = stacked(jnp.concatenate([own_ref[j], peer_ref[j]], axis=1), axis=0)[1]
    return bf16_dot(left, right, NN) * scale


def predict_kernel(j, scale, m_ref, own_ref, peer_ref, *refs):
    value = term(j, scale, m_ref, own_ref, peer_ref)
    refs[-1][...] = value + refs[0][...] if len(refs) > 1 else value


def last_predict_kernel(j, scale, route, scatter, m_ref, own_ref, peer_ref, sum_ref, out_ref, total):
    total[...] = term(j, scale, m_ref, own_ref, peer_ref) + sum_ref[...]
    place, blocks = route.place(route.core(), scatter), 1 << scatter
    size = total.shape[0] // blocks
    for k in range(blocks):
        out_ref[pl.ds(pl.multiple_of((place ^ k) * size, size), size), :] = total[k * size : (k + 1) * size, :]


def core_blocks(count):
    blocks = [(i, j) for i in range(count) for j in range(i, count)]
    half = (len(blocks) + 1) // 2
    return blocks[:half], blocks[half:]


def gram_kernel(route, scale, mine_ref, other_ref, *refs):
    outs, own_ref, p, acc = refs[:-3], refs[-3], refs[-2], refs[-1]
    half, width = mine_ref.shape[0], own_ref.shape[1]
    count = 2 * half // TILE
    lists = core_blocks(count)
    parts, core = 1 << route.row_levels, route.core()
    place = route.place(core, route.row_levels)
    here = pl.ds(pl.multiple_of(core * half, half), half)
    there = pl.ds(pl.multiple_of((1 - core) * half, half), half)
    p[here, :] = mine_ref[...]
    p[there, :width] = other_ref[:, width:]
    p[there, width:] = other_ref[:, :width]
    own_ref[...] = p[:, :width]
    for n in range(len(lists[0])):
        first = lists[0][n]
        second = lists[1][min(n, len(lists[1]) - 1)]
        i = jnp.where(core == 0, first[0], second[0])
        j = jnp.where(core == 0, first[1], second[1])
        a = p[pl.ds(pl.multiple_of(i * TILE, TILE), TILE), :]
        b = p[pl.ds(pl.multiple_of(j * TILE, TILE), TILE), :]
        acc[n * TILE : (n + 1) * TILE, :] = dot(a, b, NT) * scale
    size = acc.shape[0] // parts
    for k in range(parts):
        each = parts // len(outs)
        outs[k // each][k % each * size : (k % each + 1) * size, :] = acc[pl.ds(pl.multiple_of((place ^ k) * size, 8), size), :]


def solve_kernel(route, mine_ref, other_ref, p_ref, out_ref, natural, work, stack_a, stack_b):
    n, tile = p_ref.shape[0], TILE
    width = n + p_ref.shape[1]
    count, groups, per_panel, panels = n // tile, width // tile, PANEL // 8, tile // PANEL
    parts, core = 1 << route.row_levels, route.core()
    size = mine_ref.shape[0] // parts
    for ref, number in ((mine_ref, core), (other_ref, 1 - core)):
        place = route.place(number, route.row_levels)
        for k in range(parts):
            at = pl.multiple_of((place ^ k) * size, 8)
            natural[number, pl.ds(at, size), :] = ref[k * size : (k + 1) * size, :]
    for number, blocks in enumerate(core_blocks(count)):
        for at, (i, j) in enumerate(blocks):
            work[i * tile : (i + 1) * tile, j * tile : (j + 1) * tile] = natural[number, at * tile : (at + 1) * tile, :]
    work[:, n:] = p_ref[...]
    sub = lax.broadcasted_iota(jnp.int32, (8, tile), 0)
    deep = 6 * PANEL

    def panel(b, s):
        base = b * tile + PANEL * s
        r = [
            [work[base + 8 * i : base + 8 * i + 8, c * tile : (c + 1) * tile] for c in range(b, groups)]
            for i in range(per_panel)
        ]
        scale = [jnp.zeros((8, tile), jnp.float32)] * per_panel
        cols = {}
        for j in range(PANEL):
            start = 0 if j == 0 else j + AHEAD
            if start % GROUP == 0 and start < PANEL:
                for k in range(start, start + GROUP):
                    at = PANEL * s + k
                    cols[k] = {i: jnp.broadcast_to(r[i][0][:, at : at + 1], (8, tile)) for i in range(k // 8, per_panel)}
            jb, js = j // 8, j % 8
            col = cols[j]
            pivot = jnp.broadcast_to(col[jb][js : js + 1, :], (8, tile))
            scale[jb] = jnp.where(sub == js, lax.rsqrt(pivot), scale[jb])
            inverse = 1.0 / pivot
            mult = {i: col[i] * inverse for i in range(jb, per_panel)}
            mult[jb] = jnp.where(sub > js, mult[jb], 0.0)
            first = jb if js < 7 else jb + 1
            for k in range(j + 1, len(cols)):
                row = jnp.broadcast_to(col[k // 8][k % 8 : k % 8 + 1, :], (8, tile))
                for i in range(k // 8, per_panel):
                    cols[k][i] = cols[k][i] - mult[i] * row
            for c in range(groups - b):
                row = jnp.broadcast_to(r[jb][c][js : js + 1, :], (8, tile))
                for i in range(first, per_panel):
                    r[i][c] = r[i][c] - mult[i] * row
        return jnp.concatenate(
            [jnp.concatenate([x * scale[i] for x in r[i]], axis=1) for i in range(per_panel)], axis=0
        )

    for b in range(count):
        start = b * tile
        for s in range(panels):
            u = panel(b, s)
            out_ref[start + PANEL * s : start + PANEL * (s + 1), :] = u[:, n - start :]
            if b == count - 1 and s == panels - 1:
                break
            left, right = stacked(u, axis=0)
            if s < panels - 1:
                flipped = jnp.transpose(left[:, :tile])
                low, high, near = PANEL * (s + 1), PANEL * (s + 2), min(start + 2 * tile, width)
                for rows, columns in (((low, high), (start, near)), ((low, high), (near, width)), ((high, tile), (start, width))):
                    if rows[0] < rows[1] and columns[0] < columns[1]:
                        work[start + rows[0] : start + rows[1], columns[0] : columns[1]] -= bf16_dot(
                            flipped[rows[0] : rows[1], :], right[:, columns[0] - start : columns[1] - start], NN
                        )
            if b < count - 1:
                stack_a[deep * s : deep * (s + 1), start:n] = left[:, : n - start]
                stack_b[deep * s : deep * (s + 1), start:] = right
        for i in range(b + 1, count):
            at = i * tile
            work[at : at + tile, at:] -= bf16_dot(stack_a[:, at : at + tile], stack_b[:, at:], TN)


VMEM = pl.BlockSpec(memory_space=pltpu.VMEM)


def f32(*shape):
    return jax.ShapeDtypeStruct(shape, jnp.float32)


def call(kernel, out_shape, scratch, args):
    return pl.pallas_call(
        kernel,
        out_shape=out_shape,
        in_specs=[VMEM] * len(args),
        out_specs=jax.tree.map(lambda _: VMEM, out_shape),
        scratch_shapes=[pltpu.VMEM(s.shape, s.dtype) for s in scratch],
        compiler_params=pltpu.CompilerParams(vmem_limit_bytes=VMEM_LIMIT),
    )(*args)


def on_device(rows, cols, history):
    return orbitals(rows, cols, history)


def orbitals(rows, cols, history):
    route = Route(rows, cols)
    terms, norb, width = history.shape
    total = width * rows * cols
    half = norb // 2

    levels, scatter = route.levels, route.scatter(norb)

    peer = swap(history, route.core_perm())
    own = pl.pallas_call(
        fetch_kernel,
        name="fetch",
        out_shape=f32(*history.shape),
        in_specs=[pl.BlockSpec(memory_space=pl.ANY)],
        out_specs=VMEM,
        compiler_params=pltpu.CompilerParams(vmem_limit_bytes=VMEM_LIMIT),
    )(history)
    out = [f32(half // 2, norb)] * 2
    keep, send, left = call(
        functools.partial(first_project_kernel, route, scatter),
        out + [jax.ShapeDtypeStruct((half, 12 * width), jnp.bfloat16)],
        [f32(half, 2 * width)],
        [own, peer],
    )
    products = [(keep, send)]
    for j in range(1, terms):
        products.append(call(functools.partial(project_kernel, j), out, [], [left, own, peer]))
    m = [all_reduce(route, keep, send, scatter, levels) for keep, send in products]
    out, mine = f32(half, 2 * width), []
    for j in range(terms - 1):
        kernel = functools.partial(predict_kernel, j, WEIGHTS[j] / total)
        mine = [call(kernel, out, [], [m[j], own, peer] + mine)]
    kernel = functools.partial(last_predict_kernel, terms - 1, WEIGHTS[terms - 1] / total, route, scatter)
    mine = call(kernel, out, [out], [m[-1], own, peer] + mine)
    other = swap(mine, route.core_perm())

    shares = (norb // TILE) * (norb // TILE + 1) // 2
    share = (shares + 1) // 2 * TILE
    ways = 1 << min(2, route.row_levels)
    *pieces, predicted = call(
        functools.partial(gram_kernel, route, 1.0 / total),
        [f32(share // ways, TILE)] * ways + [f32(norb, width)],
        [f32(norb, 2 * width), f32(share, TILE)],
        [mine, other],
    )
    gram = direct_all_reduce(route, pieces, route.row_levels, levels)
    gram_other = swap(gram, route.core_perm())
    return call(
        functools.partial(solve_kernel, route),
        f32(norb, width),
        [
            f32(2, share, TILE),
            f32(norb, norb + width),
            jax.ShapeDtypeStruct((6 * TILE, norb), jnp.bfloat16),
            jax.ShapeDtypeStruct((6 * TILE, norb + width), jnp.bfloat16),
        ],
        [gram, gram_other, predicted],
    )


def solution(mesh):
    rows, cols = mesh.shape["row"], mesh.shape["col"]

    def program(history):
        step = jax.shard_map(
            functools.partial(on_device, rows, cols),
            mesh=mesh,
            in_specs=(P(None, None, AXES),),
            out_specs=P(None, AXES),
            check_vma=False,
        )
        return step(history)

    return program
```

```python
import functools

import jax
import jax.numpy as jnp
from jax import lax
from jax.experimental import pallas as pl
from jax.experimental.pallas import tpu as pltpu
from jax.sharding import PartitionSpec as P


HIGHEST = lax.Precision.HIGHEST
WEIGHTS = (2.5, -2.0, 0.5)
TILE = 128
PANEL = 32
GROUP = 16
AHEAD = 4
VMEM_LIMIT = 16 << 20
AXES = ("row", "col")
NT = (((1,), (1,)), ((), ()))
NN = (((1,), (0,)), ((), ()))
TN = (((0,), (0,)), ((), ()))


def dot(a, b, dims):
    return lax.dot_general(a, b, dims, precision=HIGHEST, preferred_element_type=jnp.float32)


def bf16_dot(a, b, dims):
    return lax.dot_general(a, b, dims, preferred_element_type=jnp.float32)


def split(x):
    high = x.astype(jnp.bfloat16)
    rest = x - high.astype(jnp.float32)
    middle = rest.astype(jnp.bfloat16)
    return high, middle, (rest - middle.astype(jnp.float32)).astype(jnp.bfloat16)


def stacked(x, axis):
    h, m, low = split(x)
    return jnp.concatenate([h, h, m, h, low, m], axis=axis), jnp.concatenate([h, m, h, low, h, m], axis=axis)


class Route:
    def __init__(self, mesh_rows, mesh_cols):
        self.rows, self.cols = mesh_rows, mesh_cols
        row_bits = list(range(1, mesh_rows.bit_length() - 1))
        col_bits = list(range(mesh_cols.bit_length() - 1))
        half = len(row_bits) // 2
        orders = (row_bits, row_bits[half:] + row_bits[:half])
        self.row_levels = len(row_bits)
        self.orders = tuple(
            [("row", b) for b in order] + [("col", b) for b in col_bits] for order in orders
        )
        self.levels = len(self.orders[0])

    def scatter(self, norb):
        return min(self.levels, (norb // 16).bit_length() - 1)

    def core(self):
        return lax.axis_index("row") & 1

    def core_perm(self):
        c = self.cols
        return [(r * c + k, (r ^ 1) * c + k) for r in range(self.rows) for k in range(c)]

    def perm(self, *levels):
        pairs = []
        for r in range(self.rows):
            for k in range(self.cols):
                flip = {"row": 0, "col": 0}
                for level in levels:
                    axis, bit = self.orders[r & 1][level]
                    flip[axis] ^= 1 << bit
                pairs.append((r * self.cols + k, (r ^ flip["row"]) * self.cols + (k ^ flip["col"])))
        return pairs

    def perms(self, first, count):
        return [
            self.perm(*[first + i for i in range(count) if q >> (count - 1 - i) & 1]) for q in range(1, 1 << count)
        ]

    def place(self, core, levels):
        index = {"row": lax.axis_index("row"), "col": lax.axis_index("col")}
        numbers = []
        for order in self.orders:
            number = jnp.int32(0)
            for axis, bit in order[:levels]:
                number = number * 2 + ((index[axis] >> bit) & 1)
            numbers.append(number)
        return jnp.where(core == 0, numbers[0], numbers[1])


def swap(x, perm):
    return lax.ppermute(x, AXES, perm)


def all_reduce(route, keep, send, scatter, levels):
    def step(x, level):
        return swap(x, route.perm(level))

    for level in range(scatter):
        got = step(send, level)
        if level < scatter - 1:
            half = keep.shape[0] // 2
            keep, send = keep[:half] + got[:half], keep[half:] + got[half:]
        else:
            keep = keep + got
    for level in range(scatter, levels):
        keep = keep + step(keep, level)
    for level in reversed(range(scatter)):
        keep = jnp.concatenate([keep, step(keep, level)], axis=0)
    return keep


def phases(first, last):
    return [(level, min(2, last - level)) for level in range(first, last, 2)]


def direct_all_reduce(route, pieces, scatter, levels):
    for number, (level, count) in enumerate(phases(0, scatter)):
        if number > 0:
            size = keep.shape[0] >> count
            pieces = [keep[q * size : (q + 1) * size] for q in range(1 << count)]
        got = [swap(piece, perm) for piece, perm in zip(pieces[1:], route.perms(level, count))]
        keep = functools.reduce(jnp.add, got, pieces[0])
    for level, count in phases(scatter, levels):
        keep = functools.reduce(jnp.add, [swap(keep, perm) for perm in route.perms(level, count)], keep)
    for level, count in reversed(phases(0, scatter)):
        keep = jnp.concatenate([keep] + [swap(keep, perm) for perm in route.perms(level, count)])
    return keep


def fetch_kernel(in_ref, out_ref):
    pltpu.sync_copy(in_ref, out_ref)


def project_kernel(j, left_ref, own_ref, peer_ref, keep_ref, send_ref):
    half = keep_ref.shape[0]
    right = stacked(jnp.concatenate([own_ref[j], peer_ref[j]], axis=1), axis=1)[1]
    keep_ref[...] = bf16_dot(left_ref[:half, :], right, NT)
    send_ref[...] = bf16_dot(left_ref[half:, :], right, NT)


def first_project_kernel(route, scatter, own_ref, peer_ref, keep_ref, send_ref, left_ref, left):
    rows, width, blocks = left.shape[0], own_ref.shape[2], 1 << scatter
    core = route.core()
    place = route.place(core, scatter)
    size = rows // blocks
    for k in range(blocks):
        at = pl.multiple_of(core * rows + (place ^ k) * size, size)
        left[k * size : (k + 1) * size, :width] = own_ref[0, pl.ds(at, size), :]
        left[k * size : (k + 1) * size, width:] = peer_ref[0, pl.ds(at, size), :]
    left_ref[...] = stacked(left[...], axis=1)[0]
    project_kernel(0, left_ref, own_ref, peer_ref, keep_ref, send_ref)


def term(j, scale, m_ref, own_ref, peer_ref):
    left = stacked(m_ref[...], axis=1)[0]
    right = stacked(jnp.concatenate([own_ref[j], peer_ref[j]], axis=1), axis=0)[1]
    return bf16_dot(left, right, NN) * scale


def predict_kernel(j, scale, m_ref, own_ref, peer_ref, *refs):
    value = term(j, scale, m_ref, own_ref, peer_ref)
    refs[-1][...] = value + refs[0][...] if len(refs) > 1 else value


def last_predict_kernel(j, scale, route, scatter, m_ref, own_ref, peer_ref, sum_ref, out_ref, total):
    total[...] = term(j, scale, m_ref, own_ref, peer_ref) + sum_ref[...]
    place, blocks = route.place(route.core(), scatter), 1 << scatter
    size = total.shape[0] // blocks
    for k in range(blocks):
        out_ref[pl.ds(pl.multiple_of((place ^ k) * size, size), size), :] = total[k * size : (k + 1) * size, :]


def core_blocks(count):
    blocks = [(i, j) for i in range(count) for j in range(i, count)]
    half = (len(blocks) + 1) // 2
    return blocks[:half], blocks[half:]


def gram_kernel(route, scale, mine_ref, other_ref, *refs):
    outs, own_ref, p, acc = refs[:-3], refs[-3], refs[-2], refs[-1]
    half, width = mine_ref.shape[0], own_ref.shape[1]
    count = 2 * half // TILE
    lists = core_blocks(count)
    parts, core = 1 << route.row_levels, route.core()
    place = route.place(core, route.row_levels)
    here = pl.ds(pl.multiple_of(core * half, half), half)
    there = pl.ds(pl.multiple_of((1 - core) * half, half), half)
    p[here, :] = mine_ref[...]
    p[there, :width] = other_ref[:, width:]
    p[there, width:] = other_ref[:, :width]
    own_ref[...] = p[:, :width]
    for n in range(len(lists[0])):
        first = lists[0][n]
        second = lists[1][min(n, len(lists[1]) - 1)]
        i = jnp.where(core == 0, first[0], second[0])
        j = jnp.where(core == 0, first[1], second[1])
        a = p[pl.ds(pl.multiple_of(i * TILE, TILE), TILE), :]
        b = p[pl.ds(pl.multiple_of(j * TILE, TILE), TILE), :]
        acc[n * TILE : (n + 1) * TILE, :] = dot(a, b, NT) * scale
    size = acc.shape[0] // parts
    for k in range(parts):
        each = parts // len(outs)
        outs[k // each][k % each * size : (k % each + 1) * size, :] = acc[pl.ds(pl.multiple_of((place ^ k) * size, 8), size), :]


def solve_kernel(route, mine_ref, other_ref, p_ref, out_ref, natural, work, stack_a, stack_b):
    n, tile = p_ref.shape[0], TILE
    width = n + p_ref.shape[1]
    count, groups, per_panel, panels = n // tile, width // tile, PANEL // 8, tile // PANEL
    parts, core = 1 << route.row_levels, route.core()
    size = mine_ref.shape[0] // parts
    for ref, number in ((mine_ref, core), (other_ref, 1 - core)):
        place = route.place(number, route.row_levels)
        for k in range(parts):
            at = pl.multiple_of((place ^ k) * size, 8)
            natural[number, pl.ds(at, size), :] = ref[k * size : (k + 1) * size, :]
    for number, blocks in enumerate(core_blocks(count)):
        for at, (i, j) in enumerate(blocks):
            work[i * tile : (i + 1) * tile, j * tile : (j + 1) * tile] = natural[number, at * tile : (at + 1) * tile, :]
    work[:, n:] = p_ref[...]
    sub = lax.broadcasted_iota(jnp.int32, (8, tile), 0)
    deep = 6 * PANEL

    def panel(b, s):
        base = b * tile + PANEL * s
        r = [
            [work[base + 8 * i : base + 8 * i + 8, c * tile : (c + 1) * tile] for c in range(b, groups)]
            for i in range(per_panel)
        ]
        scale = [jnp.zeros((8, tile), jnp.float32)] * per_panel
        cols = {}
        for j in range(PANEL):
            start = 0 if j == 0 else j + AHEAD
            if start % GROUP == 0 and start < PANEL:
                for k in range(start, start + GROUP):
                    at = PANEL * s + k
                    cols[k] = {i: jnp.broadcast_to(r[i][0][:, at : at + 1], (8, tile)) for i in range(k // 8, per_panel)}
            jb, js = j // 8, j % 8
            col = cols[j]
            pivot = jnp.broadcast_to(col[jb][js : js + 1, :], (8, tile)) if j == 0 else following
            scale[jb] = jnp.where(sub == js, lax.rsqrt(pivot), scale[jb])
            inverse = 1.0 / pivot
            below = {i: col[i] if i > jb else jnp.where(sub > js, col[i], 0.0) for i in range(jb, per_panel)}
            mult = {i: below[i] * inverse for i in range(jb, per_panel)}
            first = jb if js < 7 else jb + 1
            for k in range(j + 1, len(cols)):
                row = jnp.broadcast_to(col[k // 8][k % 8 : k % 8 + 1, :], (8, tile))
                if k == j + 1:
                    following = jnp.broadcast_to(cols[k][k // 8][k % 8 : k % 8 + 1, :], (8, tile)) - row * row * inverse
                for i in range(k // 8, per_panel):
                    cols[k][i] = cols[k][i] - mult[i] * row
            for c in range(groups - b):
                row = jnp.broadcast_to(r[jb][c][js : js + 1, :], (8, tile))
                for i in range(first, per_panel):
                    r[i][c] = r[i][c] - mult[i] * row
        return jnp.concatenate(
            [jnp.concatenate([x * scale[i] for x in r[i]], axis=1) for i in range(per_panel)], axis=0
        )

    for b in range(count):
        start = b * tile
        for s in range(panels):
            u = panel(b, s)
            out_ref[start + PANEL * s : start + PANEL * (s + 1), :] = u[:, n - start :]
            if b == count - 1 and s == panels - 1:
                break
            left, right = stacked(u, axis=0)
            if s < panels - 1:
                flipped = jnp.transpose(left[:, :tile])
                low, high, near = PANEL * (s + 1), PANEL * (s + 2), min(start + 2 * tile, width)
                for rows, columns in (((low, high), (start, near)), ((low, high), (near, width)), ((high, tile), (start, width))):
                    if rows[0] < rows[1] and columns[0] < columns[1]:
                        work[start + rows[0] : start + rows[1], columns[0] : columns[1]] -= bf16_dot(
                            flipped[rows[0] : rows[1], :], right[:, columns[0] - start : columns[1] - start], NN
                        )
            if b < count - 1:
                stack_a[deep * s : deep * (s + 1), start:n] = left[:, : n - start]
                stack_b[deep * s : deep * (s + 1), start:] = right
        for i in range(b + 1, count):
            at = i * tile
            work[at : at + tile, at:] -= bf16_dot(stack_a[:, at : at + tile], stack_b[:, at:], TN)


VMEM = pl.BlockSpec(memory_space=pltpu.VMEM)


def f32(*shape):
    return jax.ShapeDtypeStruct(shape, jnp.float32)


def call(kernel, out_shape, scratch, args, flops=0):
    moved = sum(x.size * x.dtype.itemsize for x in list(args) + jax.tree.leaves(out_shape))
    return pl.pallas_call(
        kernel,
        cost_estimate=pl.CostEstimate(flops=flops, bytes_accessed=moved, transcendentals=0),
        out_shape=out_shape,
        in_specs=[VMEM] * len(args),
        out_specs=jax.tree.map(lambda _: VMEM, out_shape),
        scratch_shapes=[pltpu.VMEM(s.shape, s.dtype) for s in scratch],
        compiler_params=pltpu.CompilerParams(vmem_limit_bytes=VMEM_LIMIT),
    )(*args)


def on_device(rows, cols, history):
    return orbitals(rows, cols, history)


def orbitals(rows, cols, history):
    route = Route(rows, cols)
    terms, norb, width = history.shape
    total = width * rows * cols
    half = norb // 2

    levels, scatter = route.levels, route.scatter(norb)

    peer = swap(history, route.core_perm())
    own = pl.pallas_call(
        fetch_kernel,
        name="fetch",
        out_shape=f32(*history.shape),
        in_specs=[pl.BlockSpec(memory_space=pl.ANY)],
        out_specs=VMEM,
        compiler_params=pltpu.CompilerParams(vmem_limit_bytes=VMEM_LIMIT),
    )(history)
    flops = 6 * 2 * half * norb * 2 * width
    out = [f32(half // 2, norb)] * 2
    keep, send, left = call(
        functools.partial(first_project_kernel, route, scatter),
        out + [jax.ShapeDtypeStruct((half, 12 * width), jnp.bfloat16)],
        [f32(half, 2 * width)],
        [own, peer],
        flops=flops,
    )
    products = [(keep, send)]
    for j in range(1, terms):
        products.append(call(functools.partial(project_kernel, j), out, [], [left, own, peer], flops))
    m = [all_reduce(route, keep, send, scatter, levels) for keep, send in products]
    out, mine = f32(half, 2 * width), []
    for j in range(terms - 1):
        kernel = functools.partial(predict_kernel, j, WEIGHTS[j] / total)
        mine = [call(kernel, out, [], [m[j], own, peer] + mine, flops)]
    kernel = functools.partial(last_predict_kernel, terms - 1, WEIGHTS[terms - 1] / total, route, scatter)
    mine = call(kernel, out, [out], [m[-1], own, peer] + mine, flops)
    other = swap(mine, route.core_perm())

    shares = (norb // TILE) * (norb // TILE + 1) // 2
    share = (shares + 1) // 2 * TILE
    ways = 1 << min(2, route.row_levels)
    *pieces, predicted = call(
        functools.partial(gram_kernel, route, 1.0 / total),
        [f32(share // ways, TILE)] * ways + [f32(norb, width)],
        [f32(norb, 2 * width), f32(share, TILE)],
        [mine, other],
    )
    gram = direct_all_reduce(route, pieces, route.row_levels, levels)
    gram_other = swap(gram, route.core_perm())
    return call(
        functools.partial(solve_kernel, route),
        f32(norb, width),
        [
            f32(2, share, TILE),
            f32(norb, norb + width),
            jax.ShapeDtypeStruct((6 * TILE, norb), jnp.bfloat16),
            jax.ShapeDtypeStruct((6 * TILE, norb + width), jnp.bfloat16),
        ],
        [gram, gram_other, predicted],
    )


def solution(mesh):
    rows, cols = mesh.shape["row"], mesh.shape["col"]

    def program(history):
        step = jax.shard_map(
            functools.partial(on_device, rows, cols),
            mesh=mesh,
            in_specs=(P(None, None, AXES),),
            out_specs=P(None, AXES),
            check_vma=False,
        )
        return step(history)

    return program
```

```python
import functools

import jax
import jax.numpy as jnp
from jax import lax
from jax.experimental import pallas as pl
from jax.experimental.pallas import tpu as pltpu
from jax.sharding import PartitionSpec as P


HIGHEST = lax.Precision.HIGHEST
WEIGHTS = (2.5, -2.0, 0.5)
TILE = 128
PANEL = 32
GROUP = 16
AHEAD = 4
VMEM_LIMIT = 16 << 20
AXES = ("row", "col")
NT = (((1,), (1,)), ((), ()))
NN = (((1,), (0,)), ((), ()))
TN = (((0,), (0,)), ((), ()))


def dot(a, b, dims):
    return lax.dot_general(a, b, dims, precision=HIGHEST, preferred_element_type=jnp.float32)


def bf16_dot(a, b, dims):
    return lax.dot_general(a, b, dims, preferred_element_type=jnp.float32)


def split(x):
    high = x.astype(jnp.bfloat16)
    rest = x - high.astype(jnp.float32)
    middle = rest.astype(jnp.bfloat16)
    return high, middle, (rest - middle.astype(jnp.float32)).astype(jnp.bfloat16)


def stacked(x, axis):
    h, m, low = split(x)
    return jnp.concatenate([h, h, m, h, low, m], axis=axis), jnp.concatenate([h, m, h, low, h, m], axis=axis)


class Route:
    def __init__(self, mesh_rows, mesh_cols):
        self.rows, self.cols = mesh_rows, mesh_cols
        row_bits = list(range(1, mesh_rows.bit_length() - 1))
        col_bits = list(range(mesh_cols.bit_length() - 1))
        half = len(row_bits) // 2
        orders = (row_bits, row_bits[half:] + row_bits[:half])
        self.row_levels = len(row_bits)
        self.orders = tuple(
            [("row", b) for b in order] + [("col", b) for b in col_bits] for order in orders
        )
        self.levels = len(self.orders[0])

    def scatter(self, norb):
        return min(self.levels, (norb // 16).bit_length() - 1)

    def core(self):
        return lax.axis_index("row") & 1

    def core_perm(self):
        c = self.cols
        return [(r * c + k, (r ^ 1) * c + k) for r in range(self.rows) for k in range(c)]

    def perm(self, *levels):
        pairs = []
        for r in range(self.rows):
            for k in range(self.cols):
                flip = {"row": 0, "col": 0}
                for level in levels:
                    axis, bit = self.orders[r & 1][level]
                    flip[axis] ^= 1 << bit
                pairs.append((r * self.cols + k, (r ^ flip["row"]) * self.cols + (k ^ flip["col"])))
        return pairs

    def perms(self, first, count):
        return [
            self.perm(*[first + i for i in range(count) if q >> (count - 1 - i) & 1]) for q in range(1, 1 << count)
        ]

    def place(self, core, levels):
        index = {"row": lax.axis_index("row"), "col": lax.axis_index("col")}
        numbers = []
        for order in self.orders:
            number = jnp.int32(0)
            for axis, bit in order[:levels]:
                number = number * 2 + ((index[axis] >> bit) & 1)
            numbers.append(number)
        return jnp.where(core == 0, numbers[0], numbers[1])


def swap(x, perm):
    return lax.ppermute(x, AXES, perm)


def all_reduce(route, keep, send, scatter, levels):
    def step(x, level):
        return swap(x, route.perm(level))

    for level in range(scatter):
        got = step(send, level)
        if level < scatter - 1:
            half = keep.shape[0] // 2
            keep, send = keep[:half] + got[:half], keep[half:] + got[half:]
        else:
            keep = lax.optimization_barrier(keep + got)
    for level in range(scatter, levels):
        keep = keep + step(keep, level)
    for level in reversed(range(scatter)):
        keep = jnp.concatenate([keep, step(keep, level)], axis=0)
    return keep


def phases(first, last):
    return [(level, min(2, last - level)) for level in range(first, last, 2)]


def direct_all_reduce(route, pieces, scatter, levels):
    for number, (level, count) in enumerate(phases(0, scatter)):
        if number > 0:
            size = keep.shape[0] >> count
            pieces = [keep[q * size : (q + 1) * size] for q in range(1 << count)]
        got = [swap(piece, perm) for piece, perm in zip(pieces[1:], route.perms(level, count))]
        keep = functools.reduce(jnp.add, got, pieces[0])
    for level, count in phases(scatter, levels):
        keep = functools.reduce(jnp.add, [swap(keep, perm) for perm in route.perms(level, count)], keep)
    for level, count in reversed(phases(0, scatter)):
        keep = jnp.concatenate([keep] + [swap(keep, perm) for perm in route.perms(level, count)])
    return keep


def fetch_kernel(in_ref, out_ref):
    pltpu.sync_copy(in_ref, out_ref)


def project_kernel(j, left_ref, own_ref, peer_ref, keep_ref, send_ref):
    half = keep_ref.shape[0]
    right = stacked(jnp.concatenate([own_ref[j], peer_ref[j]], axis=1), axis=1)[1]
    keep_ref[...] = bf16_dot(left_ref[:half, :], right, NT)
    send_ref[...] = bf16_dot(left_ref[half:, :], right, NT)


def first_project_kernel(route, scatter, own_ref, peer_ref, keep_ref, send_ref, left_ref, left, right):
    rows, width, blocks, quarter = left.shape[0], own_ref.shape[2], 1 << scatter, keep_ref.shape[0]
    core = route.core()
    place = route.place(core, scatter)
    size = rows // blocks
    for k in range(blocks):
        at = pl.multiple_of(core * rows + (place ^ k) * size, size)
        left[k * size : (k + 1) * size, :width] = own_ref[0, pl.ds(at, size), :]
        left[k * size : (k + 1) * size, width:] = peer_ref[0, pl.ds(at, size), :]
    left_ref[...] = stacked(left[...], axis=1)[0]
    right[...] = stacked(jnp.concatenate([own_ref[0], peer_ref[0]], axis=1), axis=1)[1]
    top = place >> (scatter - 1)
    for g, ref in enumerate((keep_ref, send_ref)):
        number = 2 * core + (g ^ top)
        for t in range(3):
            at = pl.multiple_of(((number + t) & 3) * quarter, quarter)
            ref[:, t * quarter : (t + 1) * quarter] = bf16_dot(
                left_ref[g * quarter : (g + 1) * quarter, :], right[pl.ds(at, quarter), :], NT
            )


def lend_kernel(route, scatter, m_ref, out_ref):
    half_blocks, quarter = 1 << (scatter - 1), out_ref.shape[0]
    place, size = route.place(route.core(), scatter), quarter // half_blocks
    for k in range(half_blocks):
        at = pl.multiple_of((place ^ (half_blocks + k)) * size, size)
        out_ref[k * size : (k + 1) * size, :] = m_ref[pl.ds(at, size), quarter : 2 * quarter]


def first_predict_kernel(scale, route, scatter, m_ref, lent_ref, own_ref, peer_ref, out_ref, x, block, turned, full):
    half_blocks, quarter, width = 1 << (scatter - 1), lent_ref.shape[0], own_ref.shape[2]
    core = route.core()
    place = route.place(core, scatter)
    top, low = place >> (scatter - 1), place & (half_blocks - 1)
    size = quarter // half_blocks
    x[:, :width] = own_ref[0]
    x[:, width:] = peer_ref[0]
    for k in range(half_blocks):
        at = pl.multiple_of((place ^ k) * size, size)
        block[k * size : (k + 1) * size, :] = m_ref[pl.ds(at, size), quarter : 2 * quarter]
    turned[0] = jnp.transpose(lent_ref[...])
    turned[1] = jnp.transpose(block[...])
    for g in range(2):
        number = 2 * core + (g ^ top)
        full[:, : 3 * quarter] = m_ref[g * quarter : (g + 1) * quarter, :]
        for k in range(half_blocks):
            at = pl.multiple_of((k ^ low) * size, size)
            full[k * size : (k + 1) * size, 3 * quarter :] = turned[g ^ top, pl.ds(at, size), :]
        parts = [x[pl.ds(pl.multiple_of(((number + t) & 3) * quarter, quarter), quarter), :] for t in range(4)]
        right = stacked(jnp.concatenate(parts, axis=0), axis=0)[1]
        out_ref[g * quarter : (g + 1) * quarter, :] = bf16_dot(stacked(full[...], axis=1)[0], right, NN) * scale


def term(j, scale, m_ref, own_ref, peer_ref):
    left = stacked(m_ref[...], axis=1)[0]
    right = stacked(jnp.concatenate([own_ref[j], peer_ref[j]], axis=1), axis=0)[1]
    return bf16_dot(left, right, NN) * scale


def predict_kernel(j, scale, m_ref, own_ref, peer_ref, *refs):
    value = term(j, scale, m_ref, own_ref, peer_ref)
    refs[-1][...] = value + refs[0][...] if len(refs) > 1 else value


def last_predict_kernel(j, scale, route, scatter, m_ref, own_ref, peer_ref, sum_ref, out_ref, total):
    total[...] = term(j, scale, m_ref, own_ref, peer_ref) + sum_ref[...]
    place, blocks = route.place(route.core(), scatter), 1 << scatter
    size = total.shape[0] // blocks
    for k in range(blocks):
        out_ref[pl.ds(pl.multiple_of((place ^ k) * size, size), size), :] = total[k * size : (k + 1) * size, :]


def core_blocks(count):
    blocks = [(i, j) for i in range(count) for j in range(i, count)]
    half = (len(blocks) + 1) // 2
    return blocks[:half], blocks[half:]


def gram_kernel(route, scale, mine_ref, other_ref, *refs):
    outs, own_ref, p, acc = refs[:-3], refs[-3], refs[-2], refs[-1]
    half, width = mine_ref.shape[0], own_ref.shape[1]
    count = 2 * half // TILE
    lists = core_blocks(count)
    parts, core = 1 << route.row_levels, route.core()
    place = route.place(core, route.row_levels)
    here = pl.ds(pl.multiple_of(core * half, half), half)
    there = pl.ds(pl.multiple_of((1 - core) * half, half), half)
    p[here, :] = mine_ref[...]
    p[there, :width] = other_ref[:, width:]
    p[there, width:] = other_ref[:, :width]
    own_ref[...] = p[:, :width]
    for n in range(len(lists[0])):
        first = lists[0][n]
        second = lists[1][min(n, len(lists[1]) - 1)]
        i = jnp.where(core == 0, first[0], second[0])
        j = jnp.where(core == 0, first[1], second[1])
        a = p[pl.ds(pl.multiple_of(i * TILE, TILE), TILE), :]
        b = p[pl.ds(pl.multiple_of(j * TILE, TILE), TILE), :]
        acc[n * TILE : (n + 1) * TILE, :] = dot(a, b, NT) * scale
    size = acc.shape[0] // parts
    for k in range(parts):
        each = parts // len(outs)
        outs[k // each][k % each * size : (k % each + 1) * size, :] = acc[pl.ds(pl.multiple_of((place ^ k) * size, 8), size), :]


def solve_kernel(route, mine_ref, other_ref, p_ref, out_ref, natural, work, stack_a, stack_b):
    n, tile = p_ref.shape[0], TILE
    width = n + p_ref.shape[1]
    count, groups, per_panel, panels = n // tile, width // tile, PANEL // 8, tile // PANEL
    parts, core = 1 << route.row_levels, route.core()
    size = mine_ref.shape[0] // parts
    for ref, number in ((mine_ref, core), (other_ref, 1 - core)):
        place = route.place(number, route.row_levels)
        for k in range(parts):
            at = pl.multiple_of((place ^ k) * size, 8)
            natural[number, pl.ds(at, size), :] = ref[k * size : (k + 1) * size, :]
    for number, blocks in enumerate(core_blocks(count)):
        for at, (i, j) in enumerate(blocks):
            work[i * tile : (i + 1) * tile, j * tile : (j + 1) * tile] = natural[number, at * tile : (at + 1) * tile, :]
    work[:, n:] = p_ref[...]
    sub = lax.broadcasted_iota(jnp.int32, (8, tile), 0)
    deep = 6 * PANEL

    def panel(b, s):
        base = b * tile + PANEL * s
        r = [
            [work[base + 8 * i : base + 8 * i + 8, c * tile : (c + 1) * tile] for c in range(b, groups)]
            for i in range(per_panel)
        ]
        scale = [jnp.zeros((8, tile), jnp.float32)] * per_panel
        cols = {}
        for j in range(PANEL):
            start = 0 if j == 0 else j + AHEAD
            if start % GROUP == 0 and start < PANEL:
                for k in range(start, start + GROUP):
                    at = PANEL * s + k
                    cols[k] = {i: jnp.broadcast_to(r[i][0][:, at : at + 1], (8, tile)) for i in range(k // 8, per_panel)}
            jb, js = j // 8, j % 8
            col = cols[j]
            pivot = jnp.broadcast_to(col[jb][js : js + 1, :], (8, tile)) if j == 0 else following
            scale[jb] = jnp.where(sub == js, lax.rsqrt(pivot), scale[jb])
            inverse = 1.0 / pivot
            below = {i: col[i] if i > jb else jnp.where(sub > js, col[i], 0.0) for i in range(jb, per_panel)}
            mult = {i: below[i] * inverse for i in range(jb, per_panel)}
            first = jb if js < 7 else jb + 1
            for k in range(j + 1, len(cols)):
                row = jnp.broadcast_to(col[k // 8][k % 8 : k % 8 + 1, :], (8, tile))
                if k == j + 1:
                    following = jnp.broadcast_to(cols[k][k // 8][k % 8 : k % 8 + 1, :], (8, tile)) - row * row * inverse
                for i in range(k // 8, per_panel):
                    cols[k][i] = cols[k][i] - mult[i] * row
            for c in range(groups - b):
                row = jnp.broadcast_to(r[jb][c][js : js + 1, :], (8, tile))
                for i in range(first, per_panel):
                    r[i][c] = r[i][c] - mult[i] * row
        return jnp.concatenate(
            [jnp.concatenate([x * scale[i] for x in r[i]], axis=1) for i in range(per_panel)], axis=0
        )

    for b in range(count):
        start = b * tile
        for s in range(panels):
            u = panel(b, s)
            out_ref[start + PANEL * s : start + PANEL * (s + 1), :] = u[:, n - start :]
            if b == count - 1 and s == panels - 1:
                break
            left, right = stacked(u, axis=0)
            if s < panels - 1:
                flipped = jnp.transpose(left[:, :tile])
                low, high, near = PANEL * (s + 1), PANEL * (s + 2), min(start + 2 * tile, width)
                for rows, columns in (((low, high), (start, near)), ((low, high), (near, width)), ((high, tile), (start, width))):
                    if rows[0] < rows[1] and columns[0] < columns[1]:
                        work[start + rows[0] : start + rows[1], columns[0] : columns[1]] -= bf16_dot(
                            flipped[rows[0] : rows[1], :], right[:, columns[0] - start : columns[1] - start], NN
                        )
            if b < count - 1:
                stack_a[deep * s : deep * (s + 1), start:n] = left[:, : n - start]
                stack_b[deep * s : deep * (s + 1), start:] = right
        for i in range(b + 1, count):
            at = i * tile
            work[at : at + tile, at:] -= bf16_dot(stack_a[:, at : at + tile], stack_b[:, at:], TN)


VMEM = pl.BlockSpec(memory_space=pltpu.VMEM)


def f32(*shape):
    return jax.ShapeDtypeStruct(shape, jnp.float32)


def call(kernel, out_shape, scratch, args, flops=0):
    moved = sum(x.size * x.dtype.itemsize for x in list(args) + jax.tree.leaves(out_shape))
    return pl.pallas_call(
        kernel,
        cost_estimate=pl.CostEstimate(flops=flops, bytes_accessed=moved, transcendentals=0),
        out_shape=out_shape,
        in_specs=[VMEM] * len(args),
        out_specs=jax.tree.map(lambda _: VMEM, out_shape),
        scratch_shapes=[pltpu.VMEM(s.shape, s.dtype) for s in scratch],
        compiler_params=pltpu.CompilerParams(vmem_limit_bytes=VMEM_LIMIT),
    )(*args)


def on_device(rows, cols, history):
    return orbitals(rows, cols, history)


def orbitals(rows, cols, history):
    route = Route(rows, cols)
    terms, norb, width = history.shape
    total = width * rows * cols
    half = norb // 2

    levels, scatter = route.levels, route.scatter(norb)

    peer = swap(history, route.core_perm())
    own = pl.pallas_call(
        fetch_kernel,
        name="fetch",
        out_shape=f32(*history.shape),
        in_specs=[pl.BlockSpec(memory_space=pl.ANY)],
        out_specs=VMEM,
        compiler_params=pltpu.CompilerParams(vmem_limit_bytes=VMEM_LIMIT),
    )(history)
    flops = 6 * 2 * half * norb * 2 * width
    out, quarter = [f32(half // 2, norb)] * 2, norb // 4
    keep, send, left = call(
        functools.partial(first_project_kernel, route, scatter),
        [f32(quarter, 3 * quarter)] * 2 + [jax.ShapeDtypeStruct((half, 12 * width), jnp.bfloat16)],
        [f32(half, 2 * width), jax.ShapeDtypeStruct((norb, 12 * width), jnp.bfloat16)],
        [own, peer],
        flops=flops,
    )
    products = [(keep, send)]
    for j in range(1, terms):
        products.append(call(functools.partial(project_kernel, j), out, [], [left, own, peer], flops))
    m = [all_reduce(route, keep, send, scatter, levels) for keep, send in products]
    out = f32(half, 2 * width)
    lent = call(functools.partial(lend_kernel, route, scatter), f32(quarter, quarter), [], [m[0]])
    lent = swap(lent, route.core_perm())
    kernel = functools.partial(first_predict_kernel, WEIGHTS[0] / total, route, scatter)
    scratch = [f32(norb, 2 * width), f32(quarter, quarter), f32(2, quarter, quarter), f32(quarter, norb)]
    mine = [call(kernel, out, scratch, [m[0], lent, own, peer], flops)]
    for j in range(1, terms - 1):
        kernel = functools.partial(predict_kernel, j, WEIGHTS[j] / total)
        mine = [call(kernel, out, [], [m[j], own, peer] + mine, flops)]
    kernel = functools.partial(last_predict_kernel, terms - 1, WEIGHTS[terms - 1] / total, route, scatter)
    mine = call(kernel, out, [out], [m[-1], own, peer] + mine, flops)
    other = swap(mine, route.core_perm())

    shares = (norb // TILE) * (norb // TILE + 1) // 2
    share = (shares + 1) // 2 * TILE
    ways = 1 << min(2, route.row_levels)
    *pieces, predicted = call(
        functools.partial(gram_kernel, route, 1.0 / total),
        [f32(share // ways, TILE)] * ways + [f32(norb, width)],
        [f32(norb, 2 * width), f32(share, TILE)],
        [mine, other],
    )
    gram = direct_all_reduce(route, pieces, route.row_levels, levels)
    gram_other = swap(gram, route.core_perm())
    return call(
        functools.partial(solve_kernel, route),
        f32(norb, width),
        [
            f32(2, share, TILE),
            f32(norb, norb + width),
            jax.ShapeDtypeStruct((6 * TILE, norb), jnp.bfloat16),
            jax.ShapeDtypeStruct((6 * TILE, norb + width), jnp.bfloat16),
        ],
        [gram, gram_other, predicted],
    )


def solution(mesh):
    rows, cols = mesh.shape["row"], mesh.shape["col"]

    def program(history):
        step = jax.shard_map(
            functools.partial(on_device, rows, cols),
            mesh=mesh,
            in_specs=(P(None, None, AXES),),
            out_specs=P(None, AXES),
            check_vma=False,
        )
        return step(history)

    return program
```

```python
import functools

import jax
import jax.numpy as jnp
from jax import lax
from jax.experimental import pallas as pl
from jax.experimental.pallas import tpu as pltpu
from jax.sharding import PartitionSpec as P


HIGHEST = lax.Precision.HIGHEST
WEIGHTS = (2.5, -2.0, 0.5)
TILE = 128
PANEL = 32
GROUP = 16
AHEAD = 4
VMEM_LIMIT = 16 << 20
AXES = ("row", "col")
NT = (((1,), (1,)), ((), ()))
NN = (((1,), (0,)), ((), ()))
TN = (((0,), (0,)), ((), ()))


def dot(a, b, dims):
    return lax.dot_general(a, b, dims, precision=HIGHEST, preferred_element_type=jnp.float32)


def bf16_dot(a, b, dims):
    return lax.dot_general(a, b, dims, preferred_element_type=jnp.float32)


def split(x):
    high = x.astype(jnp.bfloat16)
    rest = x - high.astype(jnp.float32)
    middle = rest.astype(jnp.bfloat16)
    return high, middle, (rest - middle.astype(jnp.float32)).astype(jnp.bfloat16)


def stacked(x, axis):
    h, m, low = split(x)
    return jnp.concatenate([h, h, m, h, low, m], axis=axis), jnp.concatenate([h, m, h, low, h, m], axis=axis)


class Route:
    def __init__(self, mesh_rows, mesh_cols):
        self.rows, self.cols = mesh_rows, mesh_cols
        row_bits = list(range(1, mesh_rows.bit_length() - 1))
        col_bits = list(range(mesh_cols.bit_length() - 1))
        half = len(row_bits) // 2
        orders = (row_bits, row_bits[half:] + row_bits[:half])
        self.row_levels = len(row_bits)
        self.orders = tuple(
            [("row", b) for b in order] + [("col", b) for b in col_bits] for order in orders
        )
        self.levels = len(self.orders[0])

    def scatter(self, norb):
        return min(self.levels, (norb // 16).bit_length() - 1)

    def core(self):
        return lax.axis_index("row") & 1

    def core_perm(self):
        c = self.cols
        return [(r * c + k, (r ^ 1) * c + k) for r in range(self.rows) for k in range(c)]

    def perm(self, *levels):
        pairs = []
        for r in range(self.rows):
            for k in range(self.cols):
                flip = {"row": 0, "col": 0}
                for level in levels:
                    axis, bit = self.orders[r & 1][level]
                    flip[axis] ^= 1 << bit
                pairs.append((r * self.cols + k, (r ^ flip["row"]) * self.cols + (k ^ flip["col"])))
        return pairs

    def perms(self, first, count):
        return [
            self.perm(*[first + i for i in range(count) if q >> (count - 1 - i) & 1]) for q in range(1, 1 << count)
        ]

    def place(self, core, levels):
        index = {"row": lax.axis_index("row"), "col": lax.axis_index("col")}
        numbers = []
        for order in self.orders:
            number = jnp.int32(0)
            for axis, bit in order[:levels]:
                number = number * 2 + ((index[axis] >> bit) & 1)
            numbers.append(number)
        return jnp.where(core == 0, numbers[0], numbers[1])


def swap(x, perm):
    return lax.ppermute(x, AXES, perm)


def all_reduce(route, keep, send, scatter, levels):
    def step(x, level):
        return swap(x, route.perm(level))

    for level in range(scatter):
        got = step(send, level)
        if level < scatter - 1:
            half = keep.shape[0] // 2
            keep, send = keep[:half] + got[:half], keep[half:] + got[half:]
        else:
            keep = lax.optimization_barrier(keep + got)
    for level in range(scatter, levels):
        keep = keep + step(keep, level)
    for level in reversed(range(scatter)):
        keep = jnp.concatenate([keep, step(keep, level)], axis=0)
    return keep


def phases(first, last):
    return [(level, min(2, last - level)) for level in range(first, last, 2)]


def direct_all_reduce(route, pieces, scatter, levels):
    for number, (level, count) in enumerate(phases(0, scatter)):
        if number > 0:
            size = keep.shape[0] >> count
            pieces = [keep[q * size : (q + 1) * size] for q in range(1 << count)]
        got = [swap(piece, perm) for piece, perm in zip(pieces[1:], route.perms(level, count))]
        keep = functools.reduce(jnp.add, got, pieces[0])
    for level, count in phases(scatter, levels):
        keep = functools.reduce(jnp.add, [swap(keep, perm) for perm in route.perms(level, count)], keep)
    for level, count in reversed(phases(0, scatter)):
        keep = jnp.concatenate([keep] + [swap(keep, perm) for perm in route.perms(level, count)])
    return keep


def fetch_kernel(in_ref, out_ref):
    pltpu.sync_copy(in_ref, out_ref)


def project_kernel(j, left_ref, own_ref, peer_ref, keep_ref, send_ref):
    half = keep_ref.shape[0]
    right = stacked(jnp.concatenate([own_ref[j], peer_ref[j]], axis=1), axis=1)[1]
    both = bf16_dot(left_ref[...], right, NT)
    keep_ref[...] = both[:half, :]
    send_ref[...] = both[half:, :]


def first_project_kernel(route, scatter, own_ref, peer_ref, keep_ref, send_ref, left_ref, left, right):
    rows, width, blocks, quarter = left.shape[0], own_ref.shape[2], 1 << scatter, keep_ref.shape[0]
    core = route.core()
    place = route.place(core, scatter)
    size = rows // blocks
    for k in range(blocks):
        at = pl.multiple_of(core * rows + (place ^ k) * size, size)
        left[k * size : (k + 1) * size, :width] = own_ref[0, pl.ds(at, size), :]
        left[k * size : (k + 1) * size, width:] = peer_ref[0, pl.ds(at, size), :]
    left_ref[...] = stacked(left[...], axis=1)[0]
    right[...] = stacked(jnp.concatenate([own_ref[0], peer_ref[0]], axis=1), axis=1)[1]
    top = place >> (scatter - 1)
    for g, ref in enumerate((keep_ref, send_ref)):
        number = 2 * core + (g ^ top)
        for t in range(3):
            at = pl.multiple_of(((number + t) & 3) * quarter, quarter)
            ref[:, t * quarter : (t + 1) * quarter] = bf16_dot(
                left_ref[g * quarter : (g + 1) * quarter, :], right[pl.ds(at, quarter), :], NT
            )


def lend_kernel(route, scatter, m_ref, out_ref):
    half_blocks, quarter = 1 << (scatter - 1), out_ref.shape[0]
    place, size = route.place(route.core(), scatter), quarter // half_blocks
    for k in range(half_blocks):
        at = pl.multiple_of((place ^ (half_blocks + k)) * size, size)
        out_ref[k * size : (k + 1) * size, :] = m_ref[pl.ds(at, size), quarter : 2 * quarter]


def first_predict_kernel(scale, route, scatter, m_ref, lent_ref, own_ref, peer_ref, out_ref, x, block, turned, full):
    half_blocks, quarter, width = 1 << (scatter - 1), lent_ref.shape[0], own_ref.shape[2]
    core = route.core()
    place = route.place(core, scatter)
    top, low = place >> (scatter - 1), place & (half_blocks - 1)
    size = quarter // half_blocks
    x[:, :width] = own_ref[0]
    x[:, width:] = peer_ref[0]
    for k in range(half_blocks):
        at = pl.multiple_of((place ^ k) * size, size)
        block[k * size : (k + 1) * size, :] = m_ref[pl.ds(at, size), quarter : 2 * quarter]
    turned[0] = jnp.transpose(lent_ref[...])
    turned[1] = jnp.transpose(block[...])
    for g in range(2):
        number = 2 * core + (g ^ top)
        full[:, : 3 * quarter] = m_ref[g * quarter : (g + 1) * quarter, :]
        for k in range(half_blocks):
            at = pl.multiple_of((k ^ low) * size, size)
            full[k * size : (k + 1) * size, 3 * quarter :] = turned[g ^ top, pl.ds(at, size), :]
        parts = [x[pl.ds(pl.multiple_of(((number + t) & 3) * quarter, quarter), quarter), :] for t in range(4)]
        right = stacked(jnp.concatenate(parts, axis=0), axis=0)[1]
        out_ref[g * quarter : (g + 1) * quarter, :] = bf16_dot(stacked(full[...], axis=1)[0], right, NN) * scale


def term(j, scale, m_ref, own_ref, peer_ref):
    left = stacked(m_ref[...], axis=1)[0]
    right = stacked(jnp.concatenate([own_ref[j], peer_ref[j]], axis=1), axis=0)[1]
    return bf16_dot(left, right, NN) * scale


def predict_kernel(j, scale, m_ref, own_ref, peer_ref, *refs):
    value = term(j, scale, m_ref, own_ref, peer_ref)
    refs[-1][...] = value + refs[0][...] if len(refs) > 1 else value


def last_predict_kernel(j, scale, route, scatter, m_ref, own_ref, peer_ref, sum_ref, out_ref, total):
    total[...] = term(j, scale, m_ref, own_ref, peer_ref) + sum_ref[...]
    place, blocks = route.place(route.core(), scatter), 1 << scatter
    size = total.shape[0] // blocks
    for k in range(blocks):
        out_ref[pl.ds(pl.multiple_of((place ^ k) * size, size), size), :] = total[k * size : (k + 1) * size, :]


def core_blocks(count):
    blocks = [(i, j) for i in range(count) for j in range(i, count)]
    half = (len(blocks) + 1) // 2
    return blocks[:half], blocks[half:]


def gram_kernel(route, scale, mine_ref, other_ref, *refs):
    outs, own_ref, p, acc = refs[:-3], refs[-3], refs[-2], refs[-1]
    half, width = mine_ref.shape[0], own_ref.shape[1]
    count = 2 * half // TILE
    lists = core_blocks(count)
    parts, core = 1 << route.row_levels, route.core()
    place = route.place(core, route.row_levels)
    here = pl.ds(pl.multiple_of(core * half, half), half)
    there = pl.ds(pl.multiple_of((1 - core) * half, half), half)
    p[here, :] = mine_ref[...]
    p[there, :width] = other_ref[:, width:]
    p[there, width:] = other_ref[:, :width]
    own_ref[...] = p[:, :width]
    for n in range(len(lists[0])):
        first = lists[0][n]
        second = lists[1][min(n, len(lists[1]) - 1)]
        i = jnp.where(core == 0, first[0], second[0])
        j = jnp.where(core == 0, first[1], second[1])
        a = p[pl.ds(pl.multiple_of(i * TILE, TILE), TILE), :]
        b = p[pl.ds(pl.multiple_of(j * TILE, TILE), TILE), :]
        acc[n * TILE : (n + 1) * TILE, :] = dot(a, b, NT) * scale
    size = acc.shape[0] // parts
    for k in range(parts):
        each = parts // len(outs)
        outs[k // each][k % each * size : (k % each + 1) * size, :] = acc[pl.ds(pl.multiple_of((place ^ k) * size, 8), size), :]


def solve_kernel(route, mine_ref, other_ref, p_ref, out_ref, natural, work, stack_a, stack_b):
    n, tile = p_ref.shape[0], TILE
    width = n + p_ref.shape[1]
    count, groups, per_panel, panels = n // tile, width // tile, PANEL // 8, tile // PANEL
    parts, core = 1 << route.row_levels, route.core()
    size = mine_ref.shape[0] // parts
    for ref, number in ((mine_ref, core), (other_ref, 1 - core)):
        place = route.place(number, route.row_levels)
        for k in range(parts):
            at = pl.multiple_of((place ^ k) * size, 8)
            natural[number, pl.ds(at, size), :] = ref[k * size : (k + 1) * size, :]
    for number, blocks in enumerate(core_blocks(count)):
        for at, (i, j) in enumerate(blocks):
            work[i * tile : (i + 1) * tile, j * tile : (j + 1) * tile] = natural[number, at * tile : (at + 1) * tile, :]
    work[:, n:] = p_ref[...]
    sub = lax.broadcasted_iota(jnp.int32, (8, tile), 0)
    deep = 6 * PANEL

    def panel(b, s):
        base = b * tile + PANEL * s
        r = [
            [work[base + 8 * i : base + 8 * i + 8, c * tile : (c + 1) * tile] for c in range(b, groups)]
            for i in range(per_panel)
        ]
        scale = [jnp.zeros((8, tile), jnp.float32)] * per_panel
        cols = {}
        for j in range(PANEL):
            start = 0 if j == 0 else j + AHEAD
            if start % GROUP == 0 and start < PANEL:
                for k in range(start, start + GROUP):
                    at = PANEL * s + k
                    cols[k] = {i: jnp.broadcast_to(r[i][0][:, at : at + 1], (8, tile)) for i in range(k // 8, per_panel)}
            jb, js = j // 8, j % 8
            col = cols[j]
            pivot = jnp.broadcast_to(col[jb][js : js + 1, :], (8, tile)) if j == 0 else following
            scale[jb] = jnp.where(sub == js, lax.rsqrt(pivot), scale[jb])
            inverse = 1.0 / pivot
            below = {i: col[i] if i > jb else jnp.where(sub > js, col[i], 0.0) for i in range(jb, per_panel)}
            mult = {i: below[i] * inverse for i in range(jb, per_panel)}
            first = jb if js < 7 else jb + 1
            for k in range(j + 1, len(cols)):
                row = jnp.broadcast_to(col[k // 8][k % 8 : k % 8 + 1, :], (8, tile))
                if k == j + 1:
                    following = jnp.broadcast_to(cols[k][k // 8][k % 8 : k % 8 + 1, :], (8, tile)) - row * row * inverse
                for i in range(k // 8, per_panel):
                    cols[k][i] = cols[k][i] - mult[i] * row
            for c in range(groups - b):
                row = jnp.broadcast_to(r[jb][c][js : js + 1, :], (8, tile))
                for i in range(first, per_panel):
                    r[i][c] = r[i][c] - mult[i] * row
        return jnp.concatenate(
            [jnp.concatenate([x * scale[i] for x in r[i]], axis=1) for i in range(per_panel)], axis=0
        )

    for b in range(count):
        start = b * tile
        for s in range(panels):
            u = panel(b, s)
            out_ref[start + PANEL * s : start + PANEL * (s + 1), :] = u[:, n - start :]
            if b == count - 1 and s == panels - 1:
                break
            left, right = stacked(u, axis=0)
            if s < panels - 1:
                flipped = jnp.transpose(left[:, :tile])
                low, high, near = PANEL * (s + 1), PANEL * (s + 2), min(start + 2 * tile, width)
                for rows, columns in (((low, high), (start, near)), ((low, high), (near, width)), ((high, tile), (start, width))):
                    if rows[0] < rows[1] and columns[0] < columns[1]:
                        work[start + rows[0] : start + rows[1], columns[0] : columns[1]] -= bf16_dot(
                            flipped[rows[0] : rows[1], :], right[:, columns[0] - start : columns[1] - start], NN
                        )
            if b < count - 1:
                stack_a[deep * s : deep * (s + 1), start:n] = left[:, : n - start]
                stack_b[deep * s : deep * (s + 1), start:] = right
        for i in range(b + 1, count):
            at = i * tile
            work[at : at + tile, at:] -= bf16_dot(stack_a[:, at : at + tile], stack_b[:, at:], TN)


VMEM = pl.BlockSpec(memory_space=pltpu.VMEM)


def f32(*shape):
    return jax.ShapeDtypeStruct(shape, jnp.float32)


def call(kernel, out_shape, scratch, args, flops=0):
    moved = sum(x.size * x.dtype.itemsize for x in list(args) + jax.tree.leaves(out_shape))
    return pl.pallas_call(
        kernel,
        cost_estimate=pl.CostEstimate(flops=flops, bytes_accessed=moved, transcendentals=0),
        out_shape=out_shape,
        in_specs=[VMEM] * len(args),
        out_specs=jax.tree.map(lambda _: VMEM, out_shape),
        scratch_shapes=[pltpu.VMEM(s.shape, s.dtype) for s in scratch],
        compiler_params=pltpu.CompilerParams(vmem_limit_bytes=VMEM_LIMIT),
    )(*args)


def on_device(rows, cols, history):
    return orbitals(rows, cols, history)


def orbitals(rows, cols, history):
    route = Route(rows, cols)
    terms, norb, width = history.shape
    total = width * rows * cols
    half = norb // 2

    levels, scatter = route.levels, route.scatter(norb)

    peer = swap(history, route.core_perm())
    own = pl.pallas_call(
        fetch_kernel,
        name="fetch",
        out_shape=f32(*history.shape),
        in_specs=[pl.BlockSpec(memory_space=pl.ANY)],
        out_specs=VMEM,
        compiler_params=pltpu.CompilerParams(vmem_limit_bytes=VMEM_LIMIT),
    )(history)
    flops = 6 * 2 * half * norb * 2 * width
    out, quarter = [f32(half // 2, norb)] * 2, norb // 4
    keep, send, left = call(
        functools.partial(first_project_kernel, route, scatter),
        [f32(quarter, 3 * quarter)] * 2 + [jax.ShapeDtypeStruct((half, 12 * width), jnp.bfloat16)],
        [f32(half, 2 * width), jax.ShapeDtypeStruct((norb, 12 * width), jnp.bfloat16)],
        [own, peer],
        flops=flops,
    )
    products = [(keep, send)]
    for j in range(1, terms):
        products.append(call(functools.partial(project_kernel, j), out, [], [left, own, peer], flops))
    m = [all_reduce(route, keep, send, scatter, levels) for keep, send in products]
    out = f32(half, 2 * width)
    lent = call(functools.partial(lend_kernel, route, scatter), f32(quarter, quarter), [], [m[0]])
    lent = swap(lent, route.core_perm())
    kernel = functools.partial(first_predict_kernel, WEIGHTS[0] / total, route, scatter)
    scratch = [f32(norb, 2 * width), f32(quarter, quarter), f32(2, quarter, quarter), f32(quarter, norb)]
    mine = [call(kernel, out, scratch, [m[0], lent, own, peer], flops)]
    for j in range(1, terms - 1):
        kernel = functools.partial(predict_kernel, j, WEIGHTS[j] / total)
        mine = [call(kernel, out, [], [m[j], own, peer] + mine, flops)]
    kernel = functools.partial(last_predict_kernel, terms - 1, WEIGHTS[terms - 1] / total, route, scatter)
    mine = call(kernel, out, [out], [m[-1], own, peer] + mine, flops)
    other = swap(mine, route.core_perm())

    shares = (norb // TILE) * (norb // TILE + 1) // 2
    share = (shares + 1) // 2 * TILE
    ways = 1 << min(2, route.row_levels)
    *pieces, predicted = call(
        functools.partial(gram_kernel, route, 1.0 / total),
        [f32(share // ways, TILE)] * ways + [f32(norb, width)],
        [f32(norb, 2 * width), f32(share, TILE)],
        [mine, other],
    )
    gram = direct_all_reduce(route, pieces, route.row_levels, levels)
    gram_other = swap(gram, route.core_perm())
    return call(
        functools.partial(solve_kernel, route),
        f32(norb, width),
        [
            f32(2, share, TILE),
            f32(norb, norb + width),
            jax.ShapeDtypeStruct((6 * TILE, norb), jnp.bfloat16),
            jax.ShapeDtypeStruct((6 * TILE, norb + width), jnp.bfloat16),
        ],
        [gram, gram_other, predicted],
    )


def solution(mesh):
    rows, cols = mesh.shape["row"], mesh.shape["col"]

    def program(history):
        step = jax.shard_map(
            functools.partial(on_device, rows, cols),
            mesh=mesh,
            in_specs=(P(None, None, AXES),),
            out_specs=P(None, AXES),
            check_vma=False,
        )
        return step(history)

    return program
```

```python
import functools

import jax
import jax.numpy as jnp
from jax import lax
from jax.experimental import pallas as pl
from jax.experimental.pallas import tpu as pltpu
from jax.sharding import PartitionSpec as P


WEIGHTS = (2.5, -2.0, 0.5)
TILE = 128
PANEL = 32
GROUP = 16
AHEAD = 4
VMEM_LIMIT = 16 << 20
AXES = ("row", "col")
NT = (((1,), (1,)), ((), ()))
NN = (((1,), (0,)), ((), ()))
TN = (((0,), (0,)), ((), ()))


def bf16_dot(a, b, dims):
    return lax.dot_general(a, b, dims, preferred_element_type=jnp.float32)


def split(x):
    high = x.astype(jnp.bfloat16)
    rest = x - high.astype(jnp.float32)
    middle = rest.astype(jnp.bfloat16)
    return high, middle, (rest - middle.astype(jnp.float32)).astype(jnp.bfloat16)


def stacked(x, axis):
    h, m, low = split(x)
    return jnp.concatenate([h, h, m, h, low, m], axis=axis), jnp.concatenate([h, m, h, low, h, m], axis=axis)


class Route:
    def __init__(self, mesh_rows, mesh_cols):
        self.rows, self.cols = mesh_rows, mesh_cols
        row_bits = list(range(1, mesh_rows.bit_length() - 1))
        col_bits = list(range(mesh_cols.bit_length() - 1))
        half = len(row_bits) // 2
        orders = (row_bits, row_bits[half:] + row_bits[:half])
        self.row_levels = len(row_bits)
        self.orders = tuple(
            [("row", b) for b in order] + [("col", b) for b in col_bits] for order in orders
        )
        self.levels = len(self.orders[0])

    def scatter(self, norb):
        return min(self.levels, (norb // 16).bit_length() - 1)

    def core(self):
        return lax.axis_index("row") & 1

    def core_perm(self):
        c = self.cols
        return [(r * c + k, (r ^ 1) * c + k) for r in range(self.rows) for k in range(c)]

    def perm(self, *levels):
        pairs = []
        for r in range(self.rows):
            for k in range(self.cols):
                flip = {"row": 0, "col": 0}
                for level in levels:
                    axis, bit = self.orders[r & 1][level]
                    flip[axis] ^= 1 << bit
                pairs.append((r * self.cols + k, (r ^ flip["row"]) * self.cols + (k ^ flip["col"])))
        return pairs

    def perms(self, first, count):
        return [
            self.perm(*[first + i for i in range(count) if q >> (count - 1 - i) & 1]) for q in range(1, 1 << count)
        ]

    def place(self, core, levels):
        index = {"row": lax.axis_index("row"), "col": lax.axis_index("col")}
        numbers = []
        for order in self.orders:
            number = jnp.int32(0)
            for axis, bit in order[:levels]:
                number = number * 2 + ((index[axis] >> bit) & 1)
            numbers.append(number)
        return jnp.where(core == 0, numbers[0], numbers[1])


def swap(x, perm):
    return lax.ppermute(x, AXES, perm)


def all_reduce(route, keep, send, scatter, levels):
    def step(x, level):
        return swap(x, route.perm(level))

    for level in range(scatter):
        got = step(send, level)
        if level < scatter - 1:
            half = keep.shape[0] // 2
            keep, send = keep[:half] + got[:half], keep[half:] + got[half:]
        else:
            keep = lax.optimization_barrier(keep + got)
    for level in range(scatter, levels):
        keep = keep + step(keep, level)
    for level in reversed(range(scatter)):
        keep = jnp.concatenate([keep, step(keep, level)], axis=0)
    return keep


def phases(first, last):
    return [(level, min(2, last - level)) for level in range(first, last, 2)]


def direct_all_reduce(route, pieces, scatter, levels):
    for number, (level, count) in enumerate(phases(0, scatter)):
        if number > 0:
            size = keep.shape[0] >> count
            pieces = [keep[q * size : (q + 1) * size] for q in range(1 << count)]
        got = [swap(piece, perm) for piece, perm in zip(pieces[1:], route.perms(level, count))]
        keep = functools.reduce(jnp.add, got, pieces[0])
    for level, count in phases(scatter, levels):
        keep = functools.reduce(jnp.add, [swap(keep, perm) for perm in route.perms(level, count)], keep)
    for level, count in reversed(phases(0, scatter)):
        keep = jnp.concatenate([keep] + [swap(keep, perm) for perm in route.perms(level, count)])
    return keep


def fetch_kernel(in_ref, out_ref):
    pltpu.sync_copy(in_ref, out_ref)


def project_kernel(j, left_ref, own_ref, peer_ref, keep_ref, send_ref):
    half = keep_ref.shape[0]
    right = stacked(jnp.concatenate([own_ref[j], peer_ref[j]], axis=1), axis=1)[1]
    keep_ref[...] = bf16_dot(left_ref[:half, :], right, NT)
    send_ref[...] = bf16_dot(left_ref[half:, :], right, NT)


def first_project_kernel(route, scatter, own_ref, peer_ref, keep_ref, send_ref, left_ref, left, right):
    rows, width, blocks, quarter = left.shape[0], own_ref.shape[2], 1 << scatter, keep_ref.shape[0]
    core = route.core()
    place = route.place(core, scatter)
    size = rows // blocks
    for k in range(blocks):
        at = pl.multiple_of(core * rows + (place ^ k) * size, size)
        left[k * size : (k + 1) * size, :width] = own_ref[0, pl.ds(at, size), :]
        left[k * size : (k + 1) * size, width:] = peer_ref[0, pl.ds(at, size), :]
    left_ref[...] = stacked(left[...], axis=1)[0]
    right[...] = stacked(jnp.concatenate([own_ref[0], peer_ref[0]], axis=1), axis=1)[1]
    top = place >> (scatter - 1)
    for g, ref in enumerate((keep_ref, send_ref)):
        number = 2 * core + (g ^ top)
        for t in range(3):
            at = pl.multiple_of(((number + t) & 3) * quarter, quarter)
            ref[:, t * quarter : (t + 1) * quarter] = bf16_dot(
                left_ref[g * quarter : (g + 1) * quarter, :], right[pl.ds(at, quarter), :], NT
            )


def lend_kernel(route, scatter, m_ref, out_ref):
    half_blocks, quarter = 1 << (scatter - 1), out_ref.shape[0]
    place, size = route.place(route.core(), scatter), quarter // half_blocks
    for k in range(half_blocks):
        at = pl.multiple_of((place ^ (half_blocks + k)) * size, size)
        out_ref[k * size : (k + 1) * size, :] = m_ref[pl.ds(at, size), quarter : 2 * quarter]


def first_predict_kernel(scale, route, scatter, m_ref, lent_ref, own_ref, peer_ref, out_ref, x, block, turned, full):
    half_blocks, quarter, width = 1 << (scatter - 1), lent_ref.shape[0], own_ref.shape[2]
    core = route.core()
    place = route.place(core, scatter)
    top, low = place >> (scatter - 1), place & (half_blocks - 1)
    size = quarter // half_blocks
    x[:, :width] = own_ref[0]
    x[:, width:] = peer_ref[0]
    for k in range(half_blocks):
        at = pl.multiple_of((place ^ k) * size, size)
        block[k * size : (k + 1) * size, :] = m_ref[pl.ds(at, size), quarter : 2 * quarter]
    turned[0] = jnp.transpose(lent_ref[...])
    turned[1] = jnp.transpose(block[...])
    for g in range(2):
        number = 2 * core + (g ^ top)
        full[:, : 3 * quarter] = m_ref[g * quarter : (g + 1) * quarter, :]
        for k in range(half_blocks):
            at = pl.multiple_of((k ^ low) * size, size)
            full[k * size : (k + 1) * size, 3 * quarter :] = turned[g ^ top, pl.ds(at, size), :]
        parts = [x[pl.ds(pl.multiple_of(((number + t) & 3) * quarter, quarter), quarter), :] for t in range(4)]
        right = stacked(jnp.concatenate(parts, axis=0), axis=0)[1]
        out_ref[g * quarter : (g + 1) * quarter, :] = bf16_dot(stacked(full[...], axis=1)[0], right, NN) * scale


def term(j, scale, m_ref, own_ref, peer_ref):
    left = stacked(m_ref[...], axis=1)[0]
    right = stacked(jnp.concatenate([own_ref[j], peer_ref[j]], axis=1), axis=0)[1]
    return bf16_dot(left, right, NN) * scale


def predict_kernel(j, scale, m_ref, own_ref, peer_ref, *refs):
    value = term(j, scale, m_ref, own_ref, peer_ref)
    refs[-1][...] = value + refs[0][...] if len(refs) > 1 else value


def last_predict_kernel(j, scale, route, scatter, m_ref, own_ref, peer_ref, sum_ref, out_ref, total):
    total[...] = term(j, scale, m_ref, own_ref, peer_ref) + sum_ref[...]
    place, blocks = route.place(route.core(), scatter), 1 << scatter
    size = total.shape[0] // blocks
    for k in range(blocks):
        out_ref[pl.ds(pl.multiple_of((place ^ k) * size, size), size), :] = total[k * size : (k + 1) * size, :]


def core_blocks(count):
    blocks = [(i, j) for i in range(count) for j in range(i, count)]
    half = (len(blocks) + 1) // 2
    return blocks[:half], blocks[half:]


def gram_kernel(route, scale, mine_ref, other_ref, *refs):
    outs, own_ref, p, acc, left, right = refs[:-5], *refs[-5:]
    half, width = mine_ref.shape[0], own_ref.shape[1]
    count = 2 * half // TILE
    lists = core_blocks(count)
    parts, core = 1 << route.row_levels, route.core()
    place = route.place(core, route.row_levels)
    here = pl.ds(pl.multiple_of(core * half, half), half)
    there = pl.ds(pl.multiple_of((1 - core) * half, half), half)
    p[here, :] = mine_ref[...]
    p[there, :width] = other_ref[:, width:]
    p[there, width:] = other_ref[:, :width]
    own_ref[...] = p[:, :width]
    left[...], right[...] = stacked(p[...], axis=1)
    for n in range(len(lists[0])):
        first = lists[0][n]
        second = lists[1][min(n, len(lists[1]) - 1)]
        i = jnp.where(core == 0, first[0], second[0])
        j = jnp.where(core == 0, first[1], second[1])
        a = left[pl.ds(pl.multiple_of(i * TILE, TILE), TILE), :]
        b = right[pl.ds(pl.multiple_of(j * TILE, TILE), TILE), :]
        acc[n * TILE : (n + 1) * TILE, :] = bf16_dot(a, b, NT) * scale
    size = acc.shape[0] // parts
    for k in range(parts):
        each = parts // len(outs)
        outs[k // each][k % each * size : (k % each + 1) * size, :] = acc[pl.ds(pl.multiple_of((place ^ k) * size, 8), size), :]


def solve_kernel(route, mine_ref, other_ref, p_ref, out_ref, natural, work, stack_a, stack_b):
    n, tile = p_ref.shape[0], TILE
    width = n + p_ref.shape[1]
    count, groups, per_panel, panels = n // tile, width // tile, PANEL // 8, tile // PANEL
    parts, core = 1 << route.row_levels, route.core()
    size = mine_ref.shape[0] // parts
    for ref, number in ((mine_ref, core), (other_ref, 1 - core)):
        place = route.place(number, route.row_levels)
        for k in range(parts):
            at = pl.multiple_of((place ^ k) * size, 8)
            natural[number, pl.ds(at, size), :] = ref[k * size : (k + 1) * size, :]
    for number, blocks in enumerate(core_blocks(count)):
        for at, (i, j) in enumerate(blocks):
            work[i * tile : (i + 1) * tile, j * tile : (j + 1) * tile] = natural[number, at * tile : (at + 1) * tile, :]
    work[:, n:] = p_ref[...]
    sub = lax.broadcasted_iota(jnp.int32, (8, tile), 0)
    deep = 6 * PANEL

    def panel(b, s):
        base = b * tile + PANEL * s
        r = [
            [work[base + 8 * i : base + 8 * i + 8, c * tile : (c + 1) * tile] for c in range(b, groups)]
            for i in range(per_panel)
        ]
        scale = [jnp.zeros((8, tile), jnp.float32)] * per_panel
        cols = {}
        for j in range(PANEL):
            start = 0 if j == 0 else j + AHEAD
            if start % GROUP == 0 and start < PANEL:
                for k in range(start, start + GROUP):
                    at = PANEL * s + k
                    cols[k] = {i: jnp.broadcast_to(r[i][0][:, at : at + 1], (8, tile)) for i in range(k // 8, per_panel)}
            jb, js = j // 8, j % 8
            col = cols[j]
            pivot = jnp.broadcast_to(col[jb][js : js + 1, :], (8, tile)) if j == 0 else following
            scale[jb] = jnp.where(sub == js, lax.rsqrt(pivot), scale[jb])
            inverse = 1.0 / pivot
            below = {i: col[i] if i > jb else jnp.where(sub > js, col[i], 0.0) for i in range(jb, per_panel)}
            mult = {i: below[i] * inverse for i in range(jb, per_panel)}
            first = jb if js < 7 else jb + 1
            for k in range(j + 1, len(cols)):
                row = jnp.broadcast_to(col[k // 8][k % 8 : k % 8 + 1, :], (8, tile))
                if k == j + 1:
                    following = jnp.broadcast_to(cols[k][k // 8][k % 8 : k % 8 + 1, :], (8, tile)) - row * row * inverse
                for i in range(k // 8, per_panel):
                    cols[k][i] = cols[k][i] - mult[i] * row
            for c in range(groups - b):
                row = jnp.broadcast_to(r[jb][c][js : js + 1, :], (8, tile))
                for i in range(first, per_panel):
                    r[i][c] = r[i][c] - mult[i] * row
        return jnp.concatenate(
            [jnp.concatenate([x * scale[i] for x in r[i]], axis=1) for i in range(per_panel)], axis=0
        )

    for b in range(count):
        start = b * tile
        for s in range(panels):
            u = panel(b, s)
            out_ref[start + PANEL * s : start + PANEL * (s + 1), :] = u[:, n - start :]
            if b == count - 1 and s == panels - 1:
                break
            left, right = stacked(u, axis=0)
            if s < panels - 1:
                flipped = jnp.transpose(left[:, :tile])
                low, high, near = PANEL * (s + 1), PANEL * (s + 2), min(start + 2 * tile, width)
                for rows, columns in (((low, high), (start, near)), ((low, high), (near, width)), ((high, tile), (start, width))):
                    if rows[0] < rows[1] and columns[0] < columns[1]:
                        work[start + rows[0] : start + rows[1], columns[0] : columns[1]] -= bf16_dot(
                            flipped[rows[0] : rows[1], :], right[:, columns[0] - start : columns[1] - start], NN
                        )
            if b < count - 1:
                stack_a[deep * s : deep * (s + 1), start:n] = left[:, : n - start]
                stack_b[deep * s : deep * (s + 1), start:] = right
        for i in range(b + 1, count):
            at = i * tile
            work[at : at + tile, at:] -= bf16_dot(stack_a[:, at : at + tile], stack_b[:, at:], TN)


VMEM = pl.BlockSpec(memory_space=pltpu.VMEM)


def f32(*shape):
    return jax.ShapeDtypeStruct(shape, jnp.float32)


def call(kernel, out_shape, scratch, args, flops=0):
    moved = sum(x.size * x.dtype.itemsize for x in list(args) + jax.tree.leaves(out_shape))
    return pl.pallas_call(
        kernel,
        cost_estimate=pl.CostEstimate(flops=flops, bytes_accessed=moved, transcendentals=0),
        out_shape=out_shape,
        in_specs=[VMEM] * len(args),
        out_specs=jax.tree.map(lambda _: VMEM, out_shape),
        scratch_shapes=[pltpu.VMEM(s.shape, s.dtype) for s in scratch],
        compiler_params=pltpu.CompilerParams(vmem_limit_bytes=VMEM_LIMIT),
    )(*args)


def on_device(rows, cols, history):
    return orbitals(rows, cols, history)


def orbitals(rows, cols, history):
    route = Route(rows, cols)
    terms, norb, width = history.shape
    total = width * rows * cols
    half = norb // 2

    levels, scatter = route.levels, route.scatter(norb)

    peer = swap(history, route.core_perm())
    own = pl.pallas_call(
        fetch_kernel,
        name="fetch",
        out_shape=f32(*history.shape),
        in_specs=[pl.BlockSpec(memory_space=pl.ANY)],
        out_specs=VMEM,
        compiler_params=pltpu.CompilerParams(vmem_limit_bytes=VMEM_LIMIT),
    )(history)
    flops = 6 * 2 * half * norb * 2 * width
    out, quarter = [f32(half // 2, norb)] * 2, norb // 4
    keep, send, left = call(
        functools.partial(first_project_kernel, route, scatter),
        [f32(quarter, 3 * quarter)] * 2 + [jax.ShapeDtypeStruct((half, 12 * width), jnp.bfloat16)],
        [f32(half, 2 * width), jax.ShapeDtypeStruct((norb, 12 * width), jnp.bfloat16)],
        [own, peer],
        flops=flops,
    )
    products = [(keep, send)]
    for j in range(1, terms):
        products.append(call(functools.partial(project_kernel, j), out, [], [left, own, peer], flops))
    m = [all_reduce(route, keep, send, scatter, levels) for keep, send in products]
    out = f32(half, 2 * width)
    lent = call(functools.partial(lend_kernel, route, scatter), f32(quarter, quarter), [], [m[0]])
    lent = swap(lent, route.core_perm())
    kernel = functools.partial(first_predict_kernel, WEIGHTS[0] / total, route, scatter)
    scratch = [f32(norb, 2 * width), f32(quarter, quarter), f32(2, quarter, quarter), f32(quarter, norb)]
    mine = [call(kernel, out, scratch, [m[0], lent, own, peer], flops)]
    for j in range(1, terms - 1):
        kernel = functools.partial(predict_kernel, j, WEIGHTS[j] / total)
        mine = [call(kernel, out, [], [m[j], own, peer] + mine, flops)]
    kernel = functools.partial(last_predict_kernel, terms - 1, WEIGHTS[terms - 1] / total, route, scatter)
    mine = call(kernel, out, [out], [m[-1], own, peer] + mine, flops)
    other = swap(mine, route.core_perm())

    shares = (norb // TILE) * (norb // TILE + 1) // 2
    share = (shares + 1) // 2 * TILE
    ways = 1 << min(2, route.row_levels)
    *pieces, predicted = call(
        functools.partial(gram_kernel, route, 1.0 / total),
        [f32(share // ways, TILE)] * ways + [f32(norb, width)],
        [f32(norb, 2 * width), f32(share, TILE)] + [jax.ShapeDtypeStruct((norb, 12 * width), jnp.bfloat16)] * 2,
        [mine, other],
    )
    gram = direct_all_reduce(route, pieces, route.row_levels, levels)
    gram_other = swap(gram, route.core_perm())
    return call(
        functools.partial(solve_kernel, route),
        f32(norb, width),
        [
            f32(2, share, TILE),
            f32(norb, norb + width),
            jax.ShapeDtypeStruct((6 * TILE, norb), jnp.bfloat16),
            jax.ShapeDtypeStruct((6 * TILE, norb + width), jnp.bfloat16),
        ],
        [gram, gram_other, predicted],
    )


def solution(mesh):
    rows, cols = mesh.shape["row"], mesh.shape["col"]

    def program(history):
        step = jax.shard_map(
            functools.partial(on_device, rows, cols),
            mesh=mesh,
            in_specs=(P(None, None, AXES),),
            out_specs=P(None, AXES),
            check_vma=False,
        )
        return step(history)

    return program
```
